32 devices in a mesh: kpt: 4 (over y, x), pw: 8 (over z, core).
Axes of the slice: x: 2, y: 2, z: 4, core: 2. Of those that a mesh axis runs over, the one named last changes fastest.
Arguments:
- energies: float32 [16, 512], P('kpt', 'pw'), may hold values from 0.5 to 3
- current: float32 [2, 16, 512], P(None, 'kpt', 'pw'), may hold values from -40 to 40
- previous: float32 [2, 16, 512], P(None, 'kpt', 'pw'), may hold values from -6 to 6
- previous_beta: float32 [2], replicated, may hold values from 0.5 to 2
- pair_left: bfloat16 [16, 512, 4096], P('kpt', None, 'pw'), may hold values from -0.09375 to 0.09375
- pair_right: bfloat16 [16, 512, 4096], P('kpt', None, 'pw'), may hold values from -0.25 to 0.25
- screened: bfloat16 [16, 4096, 4096], P('kpt', 'pw'), may hold values from -0.0234375 to 0.0234375
- momentum_index: int32 [16, 16], replicated, may hold values from 0 to 15, each once within a row
Outputs:
- last_vector: float32 [2, 16, 512], P(None, 'kpt', 'pw')
- prior_vector: float32 [2, 16, 512], P(None, 'kpt', 'pw')
- alpha_terms: float32 [2, 3], replicated
- beta_terms: float32 [2, 3], replicated
The draws below stay inside these ranges and needn't reach their ends.
Inputs may be any that keep to these rules, and one draw needn't show every extreme that they name: Each row of momentum_index names every index from 0 to 15 once.
All inputs are finite; a program needn't handle non-finite values.
Results may differ from the reference program's by a relative error of at most 0.003.
Values may be sent and summed in bfloat16 or wider, within the bound.
No kernel may reach another device: no remote copies, remote signals or barrier semaphores. Data moves between devices by JAX's collectives and lax.ppermute only.
A program may use at most 128 MiB of HBM per device.

```python
import math
import jax
import jax.numpy as jnp
from jax import lax

NK = 16
NC = 512
NG = 4096
NVEC = 2
STEPS = 3


def draw_current(key, part):
    normal_part = jnp.clip(jax.random.normal(key, (NVEC, NK, NC), jnp.float32), -4.0, 4.0)
    kpoint_frac = jnp.arange(NK, dtype=jnp.float32) / NK
    band_frac = jnp.arange(NC, dtype=jnp.float32) / NC
    values = normal_part
    kpoint_scale = 10.0 ** (kpoint_frac - 0.5)
    band_scale = 10.0 ** (band_frac - 0.5)
    return values * kpoint_scale[None, :, None] * band_scale[None, None, :]


def block_scale(stream_key, shape, pieces, smallest, high):
    def one(axis_at, blocks):
        steps = jax.random.uniform(jax.random.fold_in(jax.random.fold_in(stream_key, 6), axis_at), (blocks,), jnp.float32, smallest / len(pieces), high / len(pieces))
        return jnp.repeat(jnp.exp(steps), shape[axis_at] // blocks).reshape((-1,) + (1,) * (len(shape) - axis_at - 1))

    factor_of = one(*pieces[0])
    for cut in pieces[1:]:
        factor_of = factor_of * one(*cut)
    return factor_of


def centred(stream_key, dims, scale, reach, cuts=(), held_as=jnp.bfloat16):
    values = jax.random.normal(stream_key, dims, jnp.float32) * scale
    if len(cuts) > 0:
        values = block_scale(stream_key, dims, cuts, -0.22, 0.18) * values
    return jnp.clip(values, min=-reach, max=reach).astype(held_as)


def setup_inputs(seed: int = 0) -> dict:
    key_list = jax.random.split(jax.random.key(seed), 9)
    energies = jnp.clip(0.5 + 2.5 * jax.random.uniform(key_list[0], (NK, NC), jnp.float32) ** block_scale(key_list[0], (NK, NC), ((0, 4), (1, 8)), -0.2, 0.2), 0.5, 3.0)
    current = draw_current(jax.random.fold_in(key_list[8], 71), 0)
    previous = centred(key_list[2], (NVEC, NK, NC), 1.0, 6.0, ((1, 4), (2, 8)), jnp.float32)
    previous_beta = jnp.clip(jnp.exp(jax.random.uniform(key_list[3], (NVEC,), jnp.float32, math.log(0.5), math.log(2.0))), 0.5, 2.0)
    pair_left = centred(key_list[4], (NK, NC, NG), NG ** -0.5, 0.09375, ((0, 4), (2, 8)))
    pair_right = centred(key_list[5], (NK, NC, NG), NC ** -0.5, 0.25, ((0, 4), (2, 8)))
    screened = centred(key_list[6], (NK, NG, NG), (NK * NG) ** -0.5, 0.0234375, ((0, 4), (1, 8)))
    momentum_index = jax.vmap(lambda own: jax.random.permutation(own, NK))(jax.random.split(key_list[7], NK)).reshape((NK, NK)).astype(jnp.int32)
    return dict(energies=energies, current=current, previous=previous, previous_beta=previous_beta, pair_left=pair_left, pair_right=pair_right, screened=screened, momentum_index=momentum_index)


epsilon = 1e-06

def reference(energies, current, previous, previous_beta, pair_left, pair_right, screened, momentum_index):
    entries = NK * NC
    left_float = pair_left.astype(jnp.float32)
    right_float = pair_right.astype(jnp.float32)
    vector = current
    earlier = previous
    beta_before = previous_beta
    alpha_list = []
    beta_list = []
    for turn_index in range(STEPS):
        rounded = vector.astype(jnp.bfloat16)
        density = jnp.einsum('kcg,vkc->kvg', right_float, rounded.astype(jnp.float32), precision=lax.Precision.HIGHEST).astype(jnp.bfloat16)
        columns = density.reshape(NK * NVEC, NG).T

        def add_transfer(running, qpoint):
            images = jnp.dot(screened[qpoint], columns, preferred_element_type=jnp.float32).reshape(NG, NK, NVEC)
            selector = (momentum_index == qpoint).astype(jnp.float32)
            return (running + jnp.einsum('jk,gkv->jvg', selector, images, precision=lax.Precision.HIGHEST), None)
        potential, unused = lax.scan(add_transfer, jnp.zeros((NK, NVEC, NG), jnp.float32), jnp.arange(NK, dtype=jnp.int32))
        potential_bf = potential.astype(jnp.bfloat16)
        direct = jnp.einsum('kcg,kvg->vkc', left_float, potential_bf.astype(jnp.float32), precision=lax.Precision.HIGHEST)
        applied = energies[None] * vector - direct - beta_before[:, None, None] * earlier
        alpha_now = lax.optimization_barrier(jnp.sum(vector * applied, axis=(1, 2))) / entries
        residual = applied - alpha_now[:, None, None] * vector
        beta_now = jnp.sqrt(lax.optimization_barrier(jnp.sum(residual * residual, axis=(1, 2))) / entries + epsilon)
        earlier = vector
        vector = residual / beta_now[:, None, None]
        beta_before = beta_now
        alpha_list.append(alpha_now)
        beta_list.append(beta_now)
    return (vector, earlier, jnp.stack(alpha_list, axis=1), jnp.stack(beta_list, axis=1))
```

```python
import functools

import jax
import jax.numpy as jnp
from jax import lax
from jax.experimental import pallas as pl
from jax.experimental.pallas import tpu as pltpu
from jax.sharding import PartitionSpec as P

STEPS = 3
EPSILON = 1e-06
LANES = 128
BF, F32 = jnp.bfloat16, jnp.float32


def iota(shape, axis):
    return lax.broadcasted_iota(jnp.int32, shape, axis)


def high_low(x):
    high = x.astype(BF)
    return high, (x - high.astype(F32)).astype(BF)


def three_pieces(x):
    high = x.astype(BF).astype(F32)
    rest = x - high
    middle = rest.astype(BF).astype(F32)
    return high, middle, (rest - middle).astype(BF).astype(F32)


def chain_rows(x, chains):
    rows = x.shape[0] // chains
    parts = []
    for n in range(chains):
        part = jnp.sum(x[n * rows : (n + 1) * rows], axis=(0, 1), keepdims=True)
        parts.append(jnp.broadcast_to(part, (rows, 1)))
    return jnp.concatenate(parts, axis=0)


def begin_kernel(s, mi_ref, current_ref, previous_ref, energies_ref, pick_ref, out_ref):
    rows = s.rows
    bands = energies_ref.shape[1]
    mi = mi_ref[...].astype(F32).astype(BF)
    total, nk = s.groups * rows, mi.shape[0]

    def kpoint(r):
        return (r // rows) * s.kpoints + r % s.kpoints

    def chain(r):
        return (r % rows) // s.kpoints

    left = (kpoint(iota((total, nk), 0)) == iota((total, nk), 1)).astype(F32).astype(BF)
    right = (iota((nk, total), 0) == kpoint(iota((nk, total), 1))).astype(F32).astype(BF)
    spread = jnp.dot(left, mi, preferred_element_type=F32)
    spread = jnp.dot(spread.astype(BF), right, preferred_element_type=F32)
    same = chain(iota((total, total), 0)) == chain(iota((total, total), 1))
    for q in range(s.transfers):
        wanted = (lax.axis_index("kpt") * s.transfers + q).astype(F32)
        one = jnp.where(jnp.logical_and(spread == wanted, same), 1.0, 0.0).astype(BF)
        for piece in range(3):
            at = (q * 3 + piece) * total
            pick_ref[:, at : at + total] = one
    k = s.kpoints
    for b in range(s.parts):
        for n in range(s.chains):
            out_ref[b, n * k : (n + 1) * k, :] = current_ref[n]
            out_ref[b, rows + n * k : rows + (n + 1) * k, :] = previous_ref[n]
            out_ref[b, 2 * rows + n * k : 2 * rows + (n + 1) * k, :] = energies_ref[...]


def unpack_kernel(s, gathered_ref, right_ref, packet_ref, vector_ref, earlier_ref, levels_ref):
    rows = s.rows
    for at, ref in enumerate((vector_ref, earlier_ref, levels_ref)):
        ref[...] = jnp.concatenate(
            [gathered_ref[b, at * rows : (at + 1) * rows, :] for b in range(s.parts)], axis=1
        )
    density = project(s, vector_ref[...].astype(BF), right_ref)
    send(s, density, jnp.zeros((rows, LANES), F32), packet_ref)


def project(s, x, right_ref):
    rows, bands = x.shape
    total = None
    for k in range(s.kpoints):
        own = iota((rows, bands), 0) % s.kpoints == k
        masked = jnp.where(own, x.astype(F32), 0.0).astype(BF)
        part = jnp.dot(masked, right_ref[k], preferred_element_type=F32)
        total = part if total is None else total + part
    return total


def send(s, density, sums, packet_ref):
    width = density.shape[1]
    density = density.astype(BF)
    sums = sums.astype(BF)
    for d in range(s.groups * s.parts):
        packet_ref[d, :, :width] = density
        packet_ref[d, :, width:] = sums


def apply_step(s, partial_ref, vector, earlier, levels, beta):
    direct = partial_ref[0]
    for b in range(1, s.parts):
        direct = direct + partial_ref[b]
    applied = levels * vector - direct - beta * earlier
    square = chain_rows(vector * vector, s.chains)
    cross = chain_rows(vector * applied, s.chains)
    shift = jnp.where(square > 0.0, cross / jnp.where(square > 0.0, square, 1.0), 0.0)
    shift = shift.astype(BF).astype(F32)
    work = applied - shift * vector
    sums = (
        square,
        chain_rows(work * vector, s.chains),
        chain_rows(work * work, s.chains),
        shift,
    )
    lane = iota((s.rows, LANES), 1)
    value = jnp.zeros((s.rows, LANES), F32)
    for at, item in enumerate(sums):
        value = jnp.where(lane % 4 == at, item, value)
    high, middle, low = three_pieces(value)
    packed = jnp.where(lane < 4, high, jnp.where(lane < 8, middle, low))
    return work, packed


def read_sums(s, tiles):
    square, cross, work, shift = [], [], [], []
    for tile in tiles:
        value = tile[:, 0:4] + tile[:, 4:8] + tile[:, 8:12]
        for at, into in enumerate((square, cross, work, shift)):
            into.append(value[:, at : at + 1])
    alpha = sum(c + h * q for c, h, q in zip(cross, shift, square)) / s.entries
    offsets = [h - alpha for h in shift]
    mean = sum(
        w + 2.0 * o * c + o * (o * q) for w, o, c, q in zip(work, offsets, cross, square)
    )
    beta = jnp.sqrt(jnp.maximum(mean / s.entries, 0.0) + EPSILON)
    return alpha, beta, offsets


def later_kernel(
    s, partial_ref, work_ref, vector_ref, levels_ref, scalars_ref, right_ref,
    packet_ref, new_work_ref, new_vector_ref
):
    vector, beta = advance(work_ref, vector_ref, scalars_ref)
    new_vector_ref[...] = vector
    work, packed = apply_step(s, partial_ref, vector, vector_ref[...], levels_ref[...], beta)
    new_work_ref[...] = work
    finish_packet(s, work, packed, right_ref, packet_ref)


def first_kernel(
    s, partial_ref, vector_ref, earlier_ref, levels_ref, beta_ref, right_ref,
    packet_ref, new_work_ref
):
    beta = first_beta(s, beta_ref)
    work, packed = apply_step(
        s, partial_ref, vector_ref[...], earlier_ref[...], levels_ref[...], beta
    )
    new_work_ref[...] = work
    finish_packet(s, work, packed, right_ref, packet_ref)


def first_beta(s, beta_ref):
    row = iota((s.rows, 1), 0) // s.kpoints
    beta = jnp.zeros((s.rows, 1), F32)
    for n in range(s.chains):
        beta = jnp.where(row == n, beta_ref[n], beta)
    return beta


def advance(work_ref, vector_ref, scalars_ref):
    beta = scalars_ref[:, 1:2]
    offset = scalars_ref[:, 2:3]
    return (work_ref[...] + offset * vector_ref[...]) / beta, beta


def finish_packet(s, work, packed, right_ref, packet_ref):
    high, low = high_low(work)
    density = project(s, high, right_ref) + project(s, low, right_ref)
    send(s, density, packed, packet_ref)


def last_kernel(
    s, partial_ref, work_ref, vector_ref, levels_ref, scalars_ref,
    packet_ref, new_work_ref, new_vector_ref
):
    vector, beta = advance(work_ref, vector_ref, scalars_ref)
    new_vector_ref[...] = vector
    work, packed = apply_step(s, partial_ref, vector, vector_ref[...], levels_ref[...], beta)
    new_work_ref[...] = work
    for a in range(s.groups):
        packet_ref[a] = packed


def end_kernel(s, sums_ref, work_ref, vector_ref, *refs):
    scalar_refs, (last_ref, prior_ref, alphas_ref, betas_ref) = refs[:-4], refs[-4:]
    alpha, beta, offsets = read_sums(s, [sums_ref[a] for a in range(s.groups)])
    offset = own_offset(s, offsets)
    vector = vector_ref[...]
    last = (work_ref[...] + offset * vector) / beta
    width = last_ref.shape[2]
    me = lax.axis_index("pw")
    k = s.kpoints
    for value, ref in ((last, last_ref), (vector, prior_ref)):
        own = jnp.zeros((s.rows, width), F32)
        for b in range(s.parts):
            own = jnp.where(me == b, value[:, b * width : (b + 1) * width], own)
        for n in range(s.chains):
            ref[n] = own[n * k : (n + 1) * k]
    alphas = [ref[:, 0:1] for ref in scalar_refs] + [alpha]
    betas = [ref[:, 1:2] for ref in scalar_refs] + [beta]
    for n in range(s.chains):
        at = slice(n * k, n * k + 1)
        alphas_ref[n : n + 1, :] = jnp.concatenate([x[at] for x in alphas], axis=1)
        betas_ref[n : n + 1, :] = jnp.concatenate([x[at] for x in betas], axis=1)


def own_offset(s, offsets):
    me = lax.axis_index("kpt")
    own = jnp.zeros_like(offsets[0])
    for a in range(s.groups):
        own = jnp.where(me == a, offsets[a], own)
    return own


def screen_kernel(s, first, keep, *refs):
    refs = list(refs)
    packet_ref = refs.pop(0)
    before_ref = None if first else refs.pop(0)
    screened_ref, pick_ref, out_ref = refs[:3]
    refs = refs[3:]
    scalars_ref = None if first else refs.pop(0)
    density_ref = refs.pop(0) if keep else None
    (columns_ref,) = refs
    rows, total = s.rows, s.groups * s.rows
    width = packet_ref.shape[2] - LANES
    if not first:
        tiles = [packet_ref[a * s.parts, :, width:].astype(F32) for a in range(s.groups)]
        alpha, beta, offsets = read_sums(s, tiles)
        scale = 1.0 / beta
        lane = iota((rows, LANES), 1)
        scalars_ref[...] = jnp.where(
            lane == 0, alpha, jnp.where(lane == 1, beta, own_offset(s, offsets))
        )
    for a in range(s.groups):
        for b in range(s.parts):
            block = packet_ref[a * s.parts + b, :, :width]
            at = (slice(a * rows, (a + 1) * rows), slice(b * width, (b + 1) * width))
            if first:
                value = block.astype(F32)
            else:
                value = (block.astype(F32) + offsets[a] * before_ref[at]) * scale
            if keep:
                density_ref[at] = value
            high = value.astype(BF)
            columns_ref[at] = high.astype(F32)
            if not first:
                low = (slice(total + a * rows, total + (a + 1) * rows), at[1])
                columns_ref[low] = value - high.astype(F32)
    columns = columns_ref[...].astype(BF)
    pieces = []
    for q in range(s.transfers):
        image = lax.dot_general(
            screened_ref[q], columns, (((1,), (1,)), ((), ())), preferred_element_type=F32
        )
        image = image.T
        if not first:
            image = image[:total] + image[total:]
        pieces.extend(three_pieces(image))
    stacked = jnp.concatenate([piece.astype(BF) for piece in pieces], axis=0)
    field = jnp.dot(pick_ref[...], stacked, preferred_element_type=F32)
    for a in range(s.groups):
        out_ref[a] = field[a * rows : (a + 1) * rows]


def field_kernel(s, first, pieces_ref, left_ref, out_ref):
    field = pieces_ref[0]
    for a in range(1, s.groups):
        field = field + pieces_ref[a]
    parts = (field.astype(BF),) if first else high_low(field)
    stacked = jnp.concatenate([p.astype(F32) for p in parts], axis=0).astype(BF)
    rows = s.rows
    direct = None
    for k in range(s.kpoints):
        image = lax.dot_general(
            stacked, left_ref[k], (((1,), (1,)), ((), ())), preferred_element_type=F32
        )
        if not first:
            image = image[:rows] + image[rows:]
        own = iota(image.shape, 0) % s.kpoints == k
        direct = jnp.where(own, image, 0.0 if direct is None else direct)
    for b in range(s.parts):
        out_ref[b] = direct


class Sizes:
    pass


VMEM = pl.BlockSpec(memory_space=pltpu.VMEM)
SMEM = pl.BlockSpec(memory_space=pltpu.SMEM)


def call(body, args, outs, name, specs=None, scratch=(), limit=24):
    return pl.pallas_call(
        body,
        out_shape=[jax.ShapeDtypeStruct(shape, dtype) for shape, dtype in outs],
        in_specs=specs or [VMEM] * len(args),
        out_specs=[VMEM] * len(outs),
        scratch_shapes=list(scratch),
        compiler_params=pltpu.CompilerParams(vmem_limit_bytes=limit * 1024 * 1024),
        name=name,
    )(*args)


def on_device(
    groups, parts,
    energies, current, previous, previous_beta, pair_left, pair_right, screened, momentum_index
):
    s = Sizes()
    s.groups, s.parts = groups, parts
    s.chains, s.kpoints, band_block = current.shape
    s.rows = s.chains * s.kpoints
    s.transfers, width, waves = screened.shape
    bands = pair_left.shape[1]
    nk = momentum_index.shape[0]
    s.entries = float(nk * bands)
    total = groups * s.rows
    state = ((s.rows, bands), F32)
    packet = ((groups * parts, s.rows, width + LANES), BF)
    both = ("kpt", "pw")

    def exchange(x, axes):
        return lax.all_to_all(x, axes, 0, 0, tiled=True)

    screened = pltpu.with_memory_space_constraint(screened, pltpu.VMEM)
    pick, start = call(
        functools.partial(begin_kernel, s),
        (momentum_index, current, previous, energies),
        [((total, s.transfers * 3 * total), BF), ((parts, 3 * s.rows, band_block), F32)],
        "begin",
    )
    start = exchange(start, "pw")
    sent, vector, earlier, levels = call(
        functools.partial(unpack_kernel, s),
        (start, pair_right),
        [packet, state, state, state],
        "unpack",
    )
    scalars = []
    density = work = None
    for step in range(STEPS):
        first, keep = step == 0, step < STEPS - 1
        got = exchange(sent, both)
        args = (got,) + (() if first else (density,)) + (screened, pick)
        outs = [((groups, s.rows, width), F32)]
        outs += [] if first else [((s.rows, LANES), F32)]
        outs += [((total, waves), F32)] if keep else []
        results = call(
            functools.partial(screen_kernel, s, first, keep),
            args,
            outs,
            "screen",
            scratch=[pltpu.VMEM((total if first else 2 * total, waves), F32)],
        )
        field = results[0]
        if not first:
            scalars.append(results[1])
        if keep:
            density = results[-1]
        (direct,) = call(
            functools.partial(field_kernel, s, first),
            (exchange(field, "kpt"), pair_left),
            [((parts, s.rows, bands), F32)],
            "field",
        )
        direct = exchange(direct, "pw")
        if first:
            sent, work = call(
                functools.partial(first_kernel, s),
                (direct, vector, earlier, levels, previous_beta, pair_right),
                [packet, state],
                "apply",
                specs=[VMEM] * 4 + [SMEM, VMEM],
            )
        elif keep:
            sent, work, vector = call(
                functools.partial(later_kernel, s),
                (direct, work, vector, levels, scalars[-1], pair_right),
                [packet, state, state],
                "apply",
            )
        else:
            sent, work, vector = call(
                functools.partial(last_kernel, s),
                (direct, work, vector, levels, scalars[-1]),
                [((groups, s.rows, LANES), F32), state, state],
                "apply",
            )
    sums = exchange(sent, "kpt")
    own = (current.shape, F32)
    terms = ((s.chains, STEPS), F32)
    return tuple(
        call(
            functools.partial(end_kernel, s),
            (sums, work, vector, *scalars),
            [own, own, terms, terms],
            "end",
        )
    )


def solution(mesh):
    return jax.shard_map(
        functools.partial(on_device, mesh.shape["kpt"], mesh.shape["pw"]),
        mesh=mesh,
        in_specs=(
            P("kpt", "pw"),
            P(None, "kpt", "pw"),
            P(None, "kpt", "pw"),
            P(),
            P("kpt", None, "pw"),
            P("kpt", None, "pw"),
            P("kpt", "pw", None),
            P(),
        ),
        out_specs=(P(None, "kpt", "pw"), P(None, "kpt", "pw"), P(), P()),
        check_vma=False,
    )
```

```python
import functools

import jax
import jax.numpy as jnp
from jax import lax
from jax.experimental import pallas as pl
from jax.experimental.pallas import tpu as pltpu
from jax.sharding import PartitionSpec as P

STEPS = 3
EPSILON = 1e-06
COVER = 5_000_000_000
LANES = 128
BF, F32 = jnp.bfloat16, jnp.float32


def iota(shape, axis):
    return lax.broadcasted_iota(jnp.int32, shape, axis)


def high_low(x):
    high = x.astype(BF)
    return high, (x - high.astype(F32)).astype(BF)


def three_pieces(x):
    high = x.astype(BF).astype(F32)
    rest = x - high
    middle = rest.astype(BF).astype(F32)
    return high, middle, (rest - middle).astype(BF).astype(F32)


def chain_rows(x, chains):
    rows = x.shape[0] // chains
    parts = []
    for n in range(chains):
        part = jnp.sum(x[n * rows : (n + 1) * rows], axis=(0, 1), keepdims=True)
        parts.append(jnp.broadcast_to(part, (rows, 1)))
    return jnp.concatenate(parts, axis=0)


def begin_kernel(s, *refs):
    sources, held, sems = refs[:4], refs[6:10], refs[10]
    pick_ref, out_ref = refs[4:6]
    started = [
        pltpu.make_async_copy(source, target, sems.at[at])
        for at, (source, target) in enumerate(zip(sources, held))
    ]
    for copy in started:
        copy.start()
    for copy in started:
        copy.wait()
    mi_ref, current_ref, previous_ref, energies_ref = held
    rows = s.rows
    both = []
    for ref in (current_ref, previous_ref):
        both.append(jnp.concatenate([ref[n] for n in range(s.chains)], axis=0))
    levels = jnp.concatenate([energies_ref[...]] * s.chains, axis=0)
    piece = jnp.concatenate(
        [jnp.concatenate(both, axis=1), jnp.concatenate([levels] * 2, axis=1)], axis=0
    )
    for b in range(s.parts):
        out_ref[b] = piece
    mi = mi_ref[...].astype(F32).astype(BF)
    total, nk = s.groups * rows, mi.shape[0]

    def kpoint(r):
        return (r // rows) * s.kpoints + r % s.kpoints

    def chain(r):
        return (r % rows) // s.kpoints

    left = (kpoint(iota((total, nk), 0)) == iota((total, nk), 1)).astype(F32).astype(BF)
    right = (iota((nk, total), 0) == kpoint(iota((nk, total), 1))).astype(F32).astype(BF)
    spread = jnp.dot(left, mi, preferred_element_type=F32)
    spread = jnp.dot(spread.astype(BF), right, preferred_element_type=F32)
    same = chain(iota((total, total), 0)) == chain(iota((total, total), 1))
    for q in range(s.transfers):
        wanted = (lax.axis_index("kpt") * s.transfers + q).astype(F32)
        one = jnp.where(jnp.logical_and(spread == wanted, same), 1.0, 0.0).astype(BF)
        for piece in range(3):
            at = (q * 3 + piece) * total
            pick_ref[:, at : at + total] = one


def unpack_kernel(s, gathered_ref, right_ref, packet_ref, vector_ref, earlier_ref, levels_ref):
    rows = s.rows
    width = gathered_ref.shape[2] // 2
    for ref, row, lane in ((vector_ref, 0, 0), (earlier_ref, 0, width), (levels_ref, rows, 0)):
        ref[...] = jnp.concatenate(
            [
                gathered_ref[b, row : row + rows, lane : lane + width]
                for b in range(s.parts)
            ],
            axis=1,
        )
    density = project(s, vector_ref[...].astype(BF), right_ref)
    send(s, density, jnp.zeros((rows, LANES), F32), packet_ref)


def project(s, x, right_ref):
    rows, bands = x.shape
    total = None
    for k in range(s.kpoints):
        own = iota((rows, bands), 0) % s.kpoints == k
        masked = jnp.where(own, x.astype(F32), 0.0).astype(BF)
        part = jnp.dot(masked, right_ref[k], preferred_element_type=F32)
        total = part if total is None else total + part
    return total


def send(s, density, sums, packet_ref):
    width = density.shape[1]
    density = density.astype(BF)
    sums = sums.astype(BF)
    for d in range(s.groups * s.parts):
        packet_ref[d, :, :width] = density
        packet_ref[d, :, width:] = sums


def apply_step(s, partial_ref, vector, earlier, levels, beta):
    direct = partial_ref[0].astype(F32)
    for b in range(1, s.parts):
        direct = direct + partial_ref[b].astype(F32)
    applied = levels * vector - direct - beta * earlier
    square = chain_rows(vector * vector, s.chains)
    cross = chain_rows(vector * applied, s.chains)
    shift = jnp.where(square > 0.0, cross / jnp.where(square > 0.0, square, 1.0), 0.0)
    shift = shift.astype(BF).astype(F32)
    work = applied - shift * vector
    sums = (
        square,
        chain_rows(work * vector, s.chains),
        chain_rows(work * work, s.chains),
        shift,
    )
    lane = iota((s.rows, LANES), 1)
    value = jnp.zeros((s.rows, LANES), F32)
    for at, item in enumerate(sums):
        value = jnp.where(lane % 4 == at, item, value)
    high, middle, low = three_pieces(value)
    packed = jnp.where(lane < 4, high, jnp.where(lane < 8, middle, low))
    return work, packed


def read_sums(s, tiles):
    square, cross, work, shift = [], [], [], []
    for tile in tiles:
        value = tile[:, 0:4] + tile[:, 4:8] + tile[:, 8:12]
        for at, into in enumerate((square, cross, work, shift)):
            into.append(value[:, at : at + 1])
    alpha = sum(c + h * q for c, h, q in zip(cross, shift, square)) / s.entries
    offsets = [h - alpha for h in shift]
    mean = sum(
        w + 2.0 * o * c + o * (o * q) for w, o, c, q in zip(work, offsets, cross, square)
    )
    beta = jnp.sqrt(jnp.maximum(mean / s.entries, 0.0) + EPSILON)
    return alpha, beta, offsets


def later_kernel(
    s, partial_ref, work_ref, vector_ref, levels_ref, scalars_ref, right_ref,
    packet_ref, new_work_ref, new_vector_ref
):
    vector, beta = advance(work_ref, vector_ref, scalars_ref)
    new_vector_ref[...] = vector
    work, packed = apply_step(s, partial_ref, vector, vector_ref[...], levels_ref[...], beta)
    new_work_ref[...] = work
    finish_packet(s, work, packed, right_ref, packet_ref)


def first_kernel(
    s, partial_ref, vector_ref, earlier_ref, levels_ref, beta_ref, right_ref,
    packet_ref, new_work_ref
):
    beta = first_beta(s, beta_ref)
    work, packed = apply_step(
        s, partial_ref, vector_ref[...], earlier_ref[...], levels_ref[...], beta
    )
    new_work_ref[...] = work
    finish_packet(s, work, packed, right_ref, packet_ref)


def first_beta(s, beta_ref):
    row = iota((s.rows, 1), 0) // s.kpoints
    beta = jnp.zeros((s.rows, 1), F32)
    for n in range(s.chains):
        beta = jnp.where(row == n, beta_ref[n], beta)
    return beta


def advance(work_ref, vector_ref, scalars_ref):
    beta = scalars_ref[:, 1:2]
    offset = scalars_ref[:, 2:3]
    return (work_ref[...] + offset * vector_ref[...]) / beta, beta


def finish_packet(s, work, packed, right_ref, packet_ref):
    high, low = high_low(work)
    density = project(s, high, right_ref) + project(s, low, right_ref)
    send(s, density, packed, packet_ref)


def last_kernel(
    s, partial_ref, work_ref, vector_ref, levels_ref, scalars_ref,
    packet_ref, new_work_ref, new_vector_ref
):
    vector, beta = advance(work_ref, vector_ref, scalars_ref)
    new_vector_ref[...] = vector
    work, packed = apply_step(s, partial_ref, vector, vector_ref[...], levels_ref[...], beta)
    new_work_ref[...] = work
    for a in range(s.groups):
        packet_ref[a] = packed


def end_kernel(s, sums_ref, work_ref, vector_ref, *refs):
    scalar_refs, (last_ref, prior_ref, alphas_ref, betas_ref) = refs[:-4], refs[-4:]
    alpha, beta, offsets = read_sums(s, [sums_ref[a] for a in range(s.groups)])
    offset = own_offset(s, offsets)
    vector = vector_ref[...]
    last = (work_ref[...] + offset * vector) / beta
    width = last_ref.shape[2]
    me = lax.axis_index("pw")
    k = s.kpoints
    for value, ref in ((last, last_ref), (vector, prior_ref)):
        own = jnp.zeros((s.rows, width), F32)
        for b in range(s.parts):
            own = jnp.where(me == b, value[:, b * width : (b + 1) * width], own)
        for n in range(s.chains):
            ref[n] = own[n * k : (n + 1) * k]
    alphas = [ref[:, 0:1] for ref in scalar_refs] + [alpha]
    betas = [ref[:, 1:2] for ref in scalar_refs] + [beta]
    for n in range(s.chains):
        at = slice(n * k, n * k + 1)
        alphas_ref[n : n + 1, :] = jnp.concatenate([x[at] for x in alphas], axis=1)
        betas_ref[n : n + 1, :] = jnp.concatenate([x[at] for x in betas], axis=1)


def own_offset(s, offsets):
    me = lax.axis_index("kpt")
    own = jnp.zeros_like(offsets[0])
    for a in range(s.groups):
        own = jnp.where(me == a, offsets[a], own)
    return own


def screen_kernel(s, first, keep, *refs):
    refs = list(refs)
    packet_ref = refs.pop(0)
    before_ref = None if first else refs.pop(0)
    screened_ref, pick_ref, out_ref = refs[:3]
    refs = refs[3:]
    scalars_ref = None if first else refs.pop(0)
    density_ref = refs.pop(0) if keep else None
    (columns_ref,) = refs
    rows, total = s.rows, s.groups * s.rows
    width = packet_ref.shape[2] - LANES
    if not first:
        tiles = [packet_ref[a * s.parts, :, width:].astype(F32) for a in range(s.groups)]
        alpha, beta, offsets = read_sums(s, tiles)
        scale = 1.0 / beta
        lane = iota((rows, LANES), 1)
        scalars_ref[...] = jnp.where(
            lane == 0, alpha, jnp.where(lane == 1, beta, own_offset(s, offsets))
        )
    for a in range(s.groups):
        for b in range(s.parts):
            block = packet_ref[a * s.parts + b, :, :width]
            at = (slice(a * rows, (a + 1) * rows), slice(b * width, (b + 1) * width))
            if first:
                value = block.astype(F32)
            else:
                value = (block.astype(F32) + offsets[a] * before_ref[at]) * scale
            if keep:
                density_ref[at] = value
            high = value.astype(BF)
            columns_ref[at] = high.astype(F32)
            if not first:
                low = (slice(total + a * rows, total + (a + 1) * rows), at[1])
                columns_ref[low] = value - high.astype(F32)
    columns = columns_ref[...].astype(BF)
    pieces = []
    for q in range(s.transfers):
        image = lax.dot_general(
            screened_ref[q], columns, (((1,), (1,)), ((), ())), preferred_element_type=F32
        )
        image = image.T
        if not first:
            image = image[:total] + image[total:]
        pieces.extend(three_pieces(image))
    stacked = jnp.concatenate([piece.astype(BF) for piece in pieces], axis=0)
    field = jnp.dot(pick_ref[...], stacked, preferred_element_type=F32)
    for a in range(s.groups):
        out_ref[a] = field[a * rows : (a + 1) * rows]


def field_kernel(s, first, pieces_ref, left_ref, out_ref):
    field = pieces_ref[0]
    for a in range(1, s.groups):
        field = field + pieces_ref[a]
    parts = (field.astype(BF),) if first else high_low(field)
    stacked = jnp.concatenate([p.astype(F32) for p in parts], axis=0).astype(BF)
    rows = s.rows
    direct = None
    for k in range(s.kpoints):
        image = lax.dot_general(
            stacked, left_ref[k], (((1,), (1,)), ((), ())), preferred_element_type=F32
        )
        if not first:
            image = image[:rows] + image[rows:]
        own = iota(image.shape, 0) % s.kpoints == k
        direct = jnp.where(own, image, 0.0 if direct is None else direct)
    for b in range(s.parts):
        out_ref[b] = direct.astype(BF)


class Sizes:
    pass


VMEM = pl.BlockSpec(memory_space=pltpu.VMEM)
HBM = pl.BlockSpec(memory_space=pltpu.HBM)
SMEM = pl.BlockSpec(memory_space=pltpu.SMEM)


def call(body, args, outs, name, specs=None, scratch=(), limit=24, cost=0):
    return pl.pallas_call(
        body,
        out_shape=[jax.ShapeDtypeStruct(shape, dtype) for shape, dtype in outs],
        in_specs=specs or [VMEM] * len(args),
        out_specs=[VMEM] * len(outs),
        scratch_shapes=list(scratch),
        compiler_params=pltpu.CompilerParams(vmem_limit_bytes=limit * 1024 * 1024),
        name=name,
        cost_estimate=pl.CostEstimate(
            flops=cost, bytes_accessed=cost // 256, transcendentals=0
        ),
    )(*args)


def on_device(
    groups, parts,
    energies, current, previous, previous_beta, pair_left, pair_right, screened, momentum_index
):
    s = Sizes()
    s.groups, s.parts = groups, parts
    s.chains, s.kpoints, band_block = current.shape
    s.rows = s.chains * s.kpoints
    s.transfers, width, waves = screened.shape
    bands = pair_left.shape[1]
    nk = momentum_index.shape[0]
    s.entries = float(nk * bands)
    total = groups * s.rows
    state = ((s.rows, bands), F32)
    packet = ((groups * parts, s.rows, width + LANES), BF)
    both = ("kpt", "pw")

    def exchange(x, axes):
        return lax.all_to_all(x, axes, 0, 0, tiled=True)

    screened = pltpu.with_memory_space_constraint(screened, pltpu.VMEM)
    inputs = tuple(
        pltpu.with_memory_space_constraint(x, pltpu.HBM)
        for x in (momentum_index, current, previous, energies)
    )
    pick, start = call(
        functools.partial(begin_kernel, s),
        inputs,
        [
            ((total, s.transfers * 3 * total), BF),
            ((parts, 2 * s.rows, 2 * band_block), F32),
        ],
        "begin",
        specs=[HBM] * len(inputs),
        scratch=[pltpu.VMEM(x.shape, x.dtype) for x in inputs]
        + [pltpu.SemaphoreType.DMA((len(inputs),))],
        cost=COVER,
    )
    start = exchange(start, "pw")
    sent, vector, earlier, levels = call(
        functools.partial(unpack_kernel, s),
        (start, pair_right),
        [packet, state, state, state],
        "unpack",
        cost=COVER,
    )
    scalars = []
    density = work = None
    for step in range(STEPS):
        first, keep = step == 0, step < STEPS - 1
        got = exchange(sent, both)
        args = (got,) + (() if first else (density,)) + (screened, pick)
        outs = [((groups, s.rows, width), F32)]
        outs += [] if first else [((s.rows, LANES), F32)]
        outs += [((total, waves), F32)] if keep else []
        results = call(
            functools.partial(screen_kernel, s, first, keep),
            args,
            outs,
            "screen",
            scratch=[pltpu.VMEM((total if first else 2 * total, waves), F32)],
        )
        field = results[0]
        if not first:
            scalars.append(results[1])
        if keep:
            density = results[-1]
        (direct,) = call(
            functools.partial(field_kernel, s, first),
            (exchange(field, "kpt"), pair_left),
            [((parts, s.rows, bands), BF)],
            "field",
        )
        direct = exchange(direct, "pw")
        if first:
            sent, work = call(
                functools.partial(first_kernel, s),
                (direct, vector, earlier, levels, previous_beta, pair_right),
                [packet, state],
                "apply",
                specs=[VMEM] * 4 + [SMEM, VMEM],
            )
        elif keep:
            sent, work, vector = call(
                functools.partial(later_kernel, s),
                (direct, work, vector, levels, scalars[-1], pair_right),
                [packet, state, state],
                "apply",
            )
        else:
            sent, work, vector = call(
                functools.partial(last_kernel, s),
                (direct, work, vector, levels, scalars[-1]),
                [((groups, s.rows, LANES), F32), state, state],
                "apply",
            )
    sums = exchange(sent, "kpt")
    own = (current.shape, F32)
    terms = ((s.chains, STEPS), F32)
    return tuple(
        call(
            functools.partial(end_kernel, s),
            (sums, work, vector, *scalars),
            [own, own, terms, terms],
            "end",
        )
    )


def solution(mesh):
    return jax.shard_map(
        functools.partial(on_device, mesh.shape["kpt"], mesh.shape["pw"]),
        mesh=mesh,
        in_specs=(
            P("kpt", "pw"),
            P(None, "kpt", "pw"),
            P(None, "kpt", "pw"),
            P(),
            P("kpt", None, "pw"),
            P("kpt", None, "pw"),
            P("kpt", "pw", None),
            P(),
        ),
        out_specs=(P(None, "kpt", "pw"), P(None, "kpt", "pw"), P(), P()),
        check_vma=False,
    )
```

```python
import functools

import jax
import jax.numpy as jnp
from jax import lax
from jax.experimental import pallas as pl
from jax.experimental.pallas import tpu as pltpu
from jax.sharding import PartitionSpec as P

STEPS = 3
EPSILON = 1e-06
COVER = 5_000_000_000
LANES = 128
CORES = 2
BF, F32 = jnp.bfloat16, jnp.float32


def iota(shape, axis):
    return lax.broadcasted_iota(jnp.int32, shape, axis)


def high_low(x):
    high = x.astype(BF)
    return high, (x - high.astype(F32)).astype(BF)


def three_pieces(x):
    high = x.astype(BF).astype(F32)
    rest = x - high
    middle = rest.astype(BF).astype(F32)
    return high, middle, (rest - middle).astype(BF).astype(F32)


def chain_rows(x, chains):
    rows = x.shape[0] // chains
    parts = []
    for n in range(chains):
        part = jnp.sum(x[n * rows : (n + 1) * rows], axis=(0, 1), keepdims=True)
        parts.append(jnp.broadcast_to(part, (rows, 1)))
    return jnp.concatenate(parts, axis=0)


def begin_kernel(s, *refs):
    sources, held, sems = refs[:4], refs[6:10], refs[10]
    pick_ref, out_ref = refs[4:6]
    started = [
        pltpu.make_async_copy(source, target, sems.at[at])
        for at, (source, target) in enumerate(zip(sources, held))
    ]
    for copy in started:
        copy.start()
    for copy in started:
        copy.wait()
    mi_ref, current_ref, previous_ref, energies_ref = held
    rows = s.rows
    both = []
    for ref in (current_ref, previous_ref):
        both.append(jnp.concatenate([ref[n] for n in range(s.chains)], axis=0))
    levels = jnp.concatenate([energies_ref[...]] * s.chains, axis=0)
    piece = jnp.concatenate(
        [jnp.concatenate(both, axis=1), jnp.concatenate([levels] * 2, axis=1)], axis=0
    )
    for b in range(s.parts):
        out_ref[b] = piece
    mi = mi_ref[...].astype(F32).astype(BF)
    total, nk = s.groups * rows, mi.shape[0]

    def kpoint(r):
        return (r // rows) * s.kpoints + r % s.kpoints

    def chain(r):
        return (r % rows) // s.kpoints

    left = (kpoint(iota((total, nk), 0)) == iota((total, nk), 1)).astype(F32).astype(BF)
    right = (iota((nk, total), 0) == kpoint(iota((nk, total), 1))).astype(F32).astype(BF)
    spread = jnp.dot(left, mi, preferred_element_type=F32)
    spread = jnp.dot(spread.astype(BF), right, preferred_element_type=F32)
    same = chain(iota((total, total), 0)) == chain(iota((total, total), 1))
    for q in range(s.transfers):
        wanted = (lax.axis_index("kpt") * s.transfers + q).astype(F32)
        one = jnp.where(jnp.logical_and(spread == wanted, same), 1.0, 0.0).astype(BF)
        for piece in range(3):
            at = (q * 3 + piece) * total
            pick_ref[:, at : at + total] = one


def unpack_kernel(s, gathered_ref, right_ref, packet_ref, vector_ref, earlier_ref, levels_ref):
    rows = s.rows
    width = gathered_ref.shape[2] // 2
    for ref, row, lane in ((vector_ref, 0, 0), (earlier_ref, 0, width), (levels_ref, rows, 0)):
        ref[...] = jnp.concatenate(
            [
                gathered_ref[b, row : row + rows, lane : lane + width]
                for b in range(s.parts)
            ],
            axis=1,
        )
    density = project(s, vector_ref[...].astype(BF), right_ref)
    send(s, density, jnp.zeros((rows, LANES), F32), packet_ref)


def project(s, x, right_ref):
    rows, bands = x.shape
    total = None
    for k in range(s.kpoints):
        own = iota((rows, bands), 0) % s.kpoints == k
        masked = jnp.where(own, x.astype(F32), 0.0).astype(BF)
        part = jnp.dot(masked, right_ref[k], preferred_element_type=F32)
        total = part if total is None else total + part
    return total


def send(s, density, sums, packet_ref):
    width = density.shape[1]
    density = density.astype(BF)
    sums = sums.astype(BF)
    for d in range(packet_ref.shape[0]):
        packet_ref[d, :, :width] = density
        packet_ref[d, :, width:] = sums


def apply_step(s, partial_ref, vector, earlier, levels, beta):
    direct = partial_ref[0].astype(F32)
    for b in range(1, s.parts):
        direct = direct + partial_ref[b].astype(F32)
    applied = levels * vector - direct - beta * earlier
    square = chain_rows(vector * vector, s.chains)
    cross = chain_rows(vector * applied, s.chains)
    shift = jnp.where(square > 0.0, cross / jnp.where(square > 0.0, square, 1.0), 0.0)
    shift = shift.astype(BF).astype(F32)
    work = applied - shift * vector
    sums = (
        square,
        chain_rows(work * vector, s.chains),
        chain_rows(work * work, s.chains),
        shift,
    )
    lane = iota((s.rows, LANES), 1)
    value = jnp.zeros((s.rows, LANES), F32)
    for at, item in enumerate(sums):
        value = jnp.where(lane % 4 == at, item, value)
    high, middle, low = three_pieces(value)
    packed = jnp.where(lane < 4, high, jnp.where(lane < 8, middle, low))
    return work, packed


def read_sums(s, tiles):
    square, cross, work, shift = [], [], [], []
    for tile in tiles:
        value = tile[:, 0:4] + tile[:, 4:8] + tile[:, 8:12]
        for at, into in enumerate((square, cross, work, shift)):
            into.append(value[:, at : at + 1])
    alpha = sum(c + h * q for c, h, q in zip(cross, shift, square)) / s.entries
    offsets = [h - alpha for h in shift]
    mean = sum(
        w + 2.0 * o * c + o * (o * q) for w, o, c, q in zip(work, offsets, cross, square)
    )
    beta = jnp.sqrt(jnp.maximum(mean / s.entries, 0.0) + EPSILON)
    return alpha, beta, offsets


def later_kernel(
    s, partial_ref, work_ref, vector_ref, levels_ref, scalars_ref, right_ref,
    packet_ref, new_work_ref, new_vector_ref
):
    vector, beta = advance(work_ref, vector_ref, scalars_ref)
    new_vector_ref[...] = vector
    work, packed = apply_step(s, partial_ref, vector, vector_ref[...], levels_ref[...], beta)
    new_work_ref[...] = work
    finish_packet(s, work, packed, right_ref, packet_ref)


def first_kernel(
    s, partial_ref, vector_ref, earlier_ref, levels_ref, beta_ref, right_ref,
    packet_ref, new_work_ref
):
    beta = first_beta(s, beta_ref)
    work, packed = apply_step(
        s, partial_ref, vector_ref[...], earlier_ref[...], levels_ref[...], beta
    )
    new_work_ref[...] = work
    finish_packet(s, work, packed, right_ref, packet_ref)


def first_beta(s, beta_ref):
    row = iota((s.rows, 1), 0) // s.kpoints
    beta = jnp.zeros((s.rows, 1), F32)
    for n in range(s.chains):
        beta = jnp.where(row == n, beta_ref[n], beta)
    return beta


def advance(work_ref, vector_ref, scalars_ref):
    beta = scalars_ref[:, 1:2]
    offset = scalars_ref[:, 2:3]
    return (work_ref[...] + offset * vector_ref[...]) / beta, beta


def finish_packet(s, work, packed, right_ref, packet_ref):
    high, low = high_low(work)
    density = project(s, high, right_ref) + project(s, low, right_ref)
    send(s, density, packed, packet_ref)


def last_kernel(
    s, partial_ref, work_ref, vector_ref, levels_ref, scalars_ref,
    packet_ref, new_work_ref, new_vector_ref
):
    vector, beta = advance(work_ref, vector_ref, scalars_ref)
    new_vector_ref[...] = vector
    work, packed = apply_step(s, partial_ref, vector, vector_ref[...], levels_ref[...], beta)
    new_work_ref[...] = work
    packet_ref[...] = packed


def end_kernel(s, *refs):
    sums, refs = [ref[...] for ref in refs[: s.groups]], refs[s.groups :]
    work_ref, vector_ref = refs[:2]
    scalar_refs, (last_ref, prior_ref, alphas_ref, betas_ref) = refs[2:-4], refs[-4:]
    mine = lax.axis_index("kpt")
    tiles = []
    for a in range(s.groups):
        tile = sums[0]
        for other in range(1, s.groups):
            tile = jnp.where((mine ^ a) == other, sums[other], tile)
        tiles.append(tile)
    alpha, beta, offsets = read_sums(s, tiles)
    offset = own_offset(s, offsets)
    vector = vector_ref[...]
    last = (work_ref[...] + offset * vector) / beta
    width = last_ref.shape[2]
    me = lax.axis_index("z") * CORES + lax.axis_index("core")
    k = s.kpoints
    for value, ref in ((last, last_ref), (vector, prior_ref)):
        own = jnp.zeros((s.rows, width), F32)
        for b in range(s.parts):
            own = jnp.where(me == b, value[:, b * width : (b + 1) * width], own)
        for n in range(s.chains):
            ref[n] = own[n * k : (n + 1) * k]
    alphas = [ref[:, 0:1] for ref in scalar_refs] + [alpha]
    betas = [ref[:, 1:2] for ref in scalar_refs] + [beta]
    for n in range(s.chains):
        at = slice(n * k, n * k + 1)
        alphas_ref[n : n + 1, :] = jnp.concatenate([x[at] for x in alphas], axis=1)
        betas_ref[n : n + 1, :] = jnp.concatenate([x[at] for x in betas], axis=1)


def own_offset(s, offsets):
    me = lax.axis_index("kpt")
    own = jnp.zeros_like(offsets[0])
    for a in range(s.groups):
        own = jnp.where(me == a, offsets[a], own)
    return own


def screen_kernel(s, first, keep, *refs):
    refs = list(refs)
    packet_refs = refs[:CORES]
    del refs[:CORES]
    before_ref = None if first else refs.pop(0)
    screened_ref, pick_ref = refs[:2]
    out_refs = refs[2 : 2 + s.groups]
    del refs[: 2 + s.groups]
    scalars_ref = None if first else refs.pop(0)
    density_ref = refs.pop(0) if keep else None
    columns_ref, field_ref = refs
    rows, total = s.rows, s.groups * s.rows
    chips = s.parts // CORES
    width = packet_refs[0].shape[2] - LANES
    core = lax.axis_index("core")
    if not first:
        tiles = [
            jnp.where(core == 0, *(ref[a * chips, :, width:].astype(F32) for ref in packet_refs))
            for a in range(s.groups)
        ]
        alpha, beta, offsets = read_sums(s, tiles)
        scale = 1.0 / beta
        lane = iota((rows, LANES), 1)
        scalars_ref[...] = jnp.where(
            lane == 0, alpha, jnp.where(lane == 1, beta, own_offset(s, offsets))
        )
    for a in range(s.groups):
        for z in range(chips):
            for c in range(CORES):
                block = packet_refs[c][a * chips + z, :, :width].astype(F32)
                part = z * CORES + (core ^ c)
                lanes = pl.ds(pl.multiple_of(part * width, width), width)
                at = (slice(a * rows, (a + 1) * rows), lanes)
                value = block
                if not first:
                    value = (value + offsets[a] * before_ref[at]) * scale
                if keep:
                    density_ref[at] = value
                high = value.astype(BF).astype(F32)
                columns_ref[at] = high
                if not first:
                    low = (slice(total + a * rows, total + (a + 1) * rows), lanes)
                    columns_ref[low] = value - high
    columns = columns_ref[...].astype(BF)
    pieces = []
    for q in range(s.transfers):
        image = lax.dot_general(
            screened_ref[q], columns, (((1,), (1,)), ((), ())), preferred_element_type=F32
        )
        image = image.T
        if not first:
            image = image[:total] + image[total:]
        pieces.extend(three_pieces(image))
    stacked = jnp.concatenate([piece.astype(BF) for piece in pieces], axis=0)
    field_ref[...] = jnp.dot(pick_ref[...], stacked, preferred_element_type=F32)
    mine = lax.axis_index("kpt")
    for a in range(s.groups):
        out_refs[a][...] = field_ref[pl.ds(pl.multiple_of((mine ^ a) * rows, rows), rows), :]


def field_kernel(s, first, *refs):
    left_ref, out_ref = refs[-2:]
    field = refs[0][...]
    for ref in refs[1:-2]:
        field = field + ref[...]
    parts = (field.astype(BF),) if first else high_low(field)
    stacked = jnp.concatenate([p.astype(F32) for p in parts], axis=0).astype(BF)
    rows = s.rows
    direct = None
    for k in range(s.kpoints):
        image = lax.dot_general(
            stacked, left_ref[k], (((1,), (1,)), ((), ())), preferred_element_type=F32
        )
        if not first:
            image = image[:rows] + image[rows:]
        own = iota(image.shape, 0) % s.kpoints == k
        direct = jnp.where(own, image, 0.0 if direct is None else direct)
    for b in range(s.parts):
        out_ref[b] = direct.astype(BF)


class Sizes:
    pass


VMEM = pl.BlockSpec(memory_space=pltpu.VMEM)
HBM = pl.BlockSpec(memory_space=pltpu.HBM)
SMEM = pl.BlockSpec(memory_space=pltpu.SMEM)


def call(body, args, outs, name, specs=None, scratch=(), limit=24, cost=0):
    return pl.pallas_call(
        body,
        out_shape=[jax.ShapeDtypeStruct(shape, dtype) for shape, dtype in outs],
        in_specs=specs or [VMEM] * len(args),
        out_specs=[VMEM] * len(outs),
        scratch_shapes=list(scratch),
        compiler_params=pltpu.CompilerParams(vmem_limit_bytes=limit * 1024 * 1024),
        name=name,
        cost_estimate=pl.CostEstimate(
            flops=cost, bytes_accessed=cost // 256, transcendentals=0
        ),
    )(*args)


def on_device(
    groups, parts,
    energies, current, previous, previous_beta, pair_left, pair_right, screened, momentum_index
):
    s = Sizes()
    s.groups, s.parts = groups, parts
    s.chains, s.kpoints, band_block = current.shape
    s.rows = s.chains * s.kpoints
    s.transfers, width, waves = screened.shape
    bands = pair_left.shape[1]
    nk = momentum_index.shape[0]
    s.entries = float(nk * bands)
    total = groups * s.rows
    state = ((s.rows, bands), F32)
    packet = ((groups * parts // CORES, s.rows, width + LANES), BF)
    chip = ("z", "core")

    def exchange(x, axes):
        return lax.all_to_all(x, axes, 0, 0, tiled=True)

    def across(x, axis, size, distance):
        return lax.ppermute(x, axis, [(i, i ^ distance) for i in range(size)])

    def swap(pieces):
        return [pieces[0]] + [
            across(piece, "kpt", groups, a) for a, piece in enumerate(pieces) if a
        ]

    screened = pltpu.with_memory_space_constraint(screened, pltpu.VMEM)
    inputs = tuple(
        pltpu.with_memory_space_constraint(x, pltpu.HBM)
        for x in (momentum_index, current, previous, energies)
    )
    pick, start = call(
        functools.partial(begin_kernel, s),
        inputs,
        [
            ((total, s.transfers * 3 * total), BF),
            ((parts, 2 * s.rows, 2 * band_block), F32),
        ],
        "begin",
        specs=[HBM] * len(inputs),
        scratch=[pltpu.VMEM(x.shape, x.dtype) for x in inputs]
        + [pltpu.SemaphoreType.DMA((len(inputs),))],
        cost=COVER,
    )
    start = exchange(start, chip)
    sent, vector, earlier, levels = call(
        functools.partial(unpack_kernel, s),
        (start, pair_right),
        [packet, state, state, state],
        "unpack",
        cost=COVER,
    )
    scalars = []
    density = work = None
    for step in range(STEPS):
        first, keep = step == 0, step < STEPS - 1
        got = exchange(sent, ("kpt", "z"))
        args = (got, across(got, "core", CORES, 1)) + (() if first else (density,)) + (screened, pick)
        outs = [((s.rows, width), F32)] * groups
        outs += [] if first else [((s.rows, LANES), F32)]
        outs += [((total, waves), F32)] if keep else []
        results = call(
            functools.partial(screen_kernel, s, first, keep),
            args,
            outs,
            "screen",
            scratch=[
                pltpu.VMEM((total if first else 2 * total, waves), F32),
                pltpu.VMEM((total, width), F32),
            ],
        )
        if not first:
            scalars.append(results[groups])
        if keep:
            density = results[-1]
        (direct,) = call(
            functools.partial(field_kernel, s, first),
            (*swap(results[:groups]), pair_left),
            [((parts, s.rows, bands), BF)],
            "field",
        )
        direct = exchange(direct, chip)
        if first:
            sent, work = call(
                functools.partial(first_kernel, s),
                (direct, vector, earlier, levels, previous_beta, pair_right),
                [packet, state],
                "apply",
                specs=[VMEM] * 4 + [SMEM, VMEM],
            )
        elif keep:
            sent, work, vector = call(
                functools.partial(later_kernel, s),
                (direct, work, vector, levels, scalars[-1], pair_right),
                [packet, state, state],
                "apply",
            )
        else:
            sent, work, vector = call(
                functools.partial(last_kernel, s),
                (direct, work, vector, levels, scalars[-1]),
                [((s.rows, LANES), F32), state, state],
                "apply",
            )
    sums = swap([sent] * groups)
    own = (current.shape, F32)
    terms = ((s.chains, STEPS), F32)
    return tuple(
        call(
            functools.partial(end_kernel, s),
            (*sums, work, vector, *scalars),
            [own, own, terms, terms],
            "end",
        )
    )


def solution(mesh):
    groups, parts = mesh.shape["kpt"], mesh.shape["pw"]
    devices = mesh.devices.reshape(groups, parts // CORES, CORES)
    pw = ("z", "core")
    return jax.shard_map(
        functools.partial(on_device, groups, parts),
        mesh=jax.sharding.Mesh(devices, ("kpt", *pw)),
        in_specs=(
            P("kpt", pw),
            P(None, "kpt", pw),
            P(None, "kpt", pw),
            P(),
            P("kpt", None, pw),
            P("kpt", None, pw),
            P("kpt", pw, None),
            P(),
        ),
        out_specs=(P(None, "kpt", pw), P(None, "kpt", pw), P(), P()),
        check_vma=False,
    )
```

```python
import functools

import jax
import jax.numpy as jnp
from jax import lax
from jax.experimental import pallas as pl
from jax.experimental.pallas import tpu as pltpu
from jax.sharding import PartitionSpec as P

STEPS = 3
EPSILON = 1e-06
COVER = 5_000_000_000
LANES = 128
CORES = 2
BF, F32 = jnp.bfloat16, jnp.float32


def iota(shape, axis):
    return lax.broadcasted_iota(jnp.int32, shape, axis)


def high_low(x):
    high = x.astype(BF)
    return high, (x - high.astype(F32)).astype(BF)


def three_pieces(x):
    high = x.astype(BF).astype(F32)
    rest = x - high
    middle = rest.astype(BF).astype(F32)
    return high, middle, (rest - middle).astype(BF).astype(F32)


def chain_rows(x, chains):
    rows = x.shape[0] // chains
    parts = []
    for n in range(chains):
        part = jnp.sum(x[n * rows : (n + 1) * rows], axis=(0, 1), keepdims=True)
        parts.append(jnp.broadcast_to(part, (rows, 1)))
    return jnp.concatenate(parts, axis=0)


def copy_all(sources, targets, sems):
    started = [
        pltpu.make_async_copy(source, target, sems.at[at])
        for at, (source, target) in enumerate(zip(sources, targets))
    ]
    for copy in started:
        copy.start()
    for copy in started:
        copy.wait()


def begin_kernel(s, *refs):
    sources, held, sems = refs[:4], refs[6:10], refs[10]
    pick_ref, out_ref = refs[4:6]
    copy_all(sources, held, sems)
    mi_ref, current_ref, previous_ref, energies_ref = held
    rows = s.rows
    both = []
    for ref in (current_ref, previous_ref):
        both.append(jnp.concatenate([ref[n] for n in range(s.chains)], axis=0))
    levels = jnp.concatenate([energies_ref[...]] * s.chains, axis=0)
    piece = jnp.concatenate(
        [jnp.concatenate(both, axis=1), jnp.concatenate([levels] * 2, axis=1)], axis=0
    )
    for b in range(s.parts):
        out_ref[b] = piece
    mi = mi_ref[...].astype(F32).astype(BF)
    total, nk = s.groups * rows, mi.shape[0]

    def kpoint(r):
        return (r // rows) * s.kpoints + r % s.kpoints

    def chain(r):
        return (r % rows) // s.kpoints

    left = (kpoint(iota((total, nk), 0)) == iota((total, nk), 1)).astype(F32).astype(BF)
    right = (iota((nk, total), 0) == kpoint(iota((nk, total), 1))).astype(F32).astype(BF)
    spread = jnp.dot(left, mi, preferred_element_type=F32)
    spread = jnp.dot(spread.astype(BF), right, preferred_element_type=F32)
    same = chain(iota((total, total), 0)) == chain(iota((total, total), 1))
    for q in range(s.transfers):
        wanted = (lax.axis_index("kpt") * s.transfers + q).astype(F32)
        one = jnp.where(jnp.logical_and(spread == wanted, same), 1.0, 0.0).astype(BF)
        for piece in range(3):
            at = (q * 3 + piece) * total
            pick_ref[:, at : at + total] = one


def unpack_kernel(s, gathered_ref, right_ref, packet_ref, vector_ref, earlier_ref, levels_ref):
    rows = s.rows
    width = gathered_ref.shape[2] // 2
    for ref, row, lane in ((vector_ref, 0, 0), (earlier_ref, 0, width), (levels_ref, rows, 0)):
        ref[...] = jnp.concatenate(
            [
                gathered_ref[b, row : row + rows, lane : lane + width]
                for b in range(s.parts)
            ],
            axis=1,
        )
    density = project(s, (vector_ref[...].astype(BF),), right_ref)
    send(s, density, jnp.zeros((rows, LANES), F32), packet_ref)


def project(s, parts, right_ref):
    x = jnp.concatenate([part.astype(F32) for part in parts], axis=0)
    total = None
    for k in range(s.kpoints):
        own = iota(x.shape, 0) % s.kpoints == k
        masked = jnp.where(own, x, 0.0).astype(BF)
        part = jnp.dot(masked, right_ref[k], preferred_element_type=F32)
        total = part if total is None else total + part
    return sum(total[at : at + s.rows] for at in range(0, x.shape[0], s.rows))


def send(s, density, sums, packet_ref):
    width = density.shape[1]
    density = density.astype(BF)
    sums = sums.astype(BF)
    for d in range(packet_ref.shape[0]):
        packet_ref[d, :, :width] = density
        packet_ref[d, :, width:] = sums


def pair_kernel(s, own_ref, other_ref, out_ref):
    out_ref[...] = (own_ref[...] + other_ref[...]).astype(BF)


def apply_step(s, refs, vector, earlier, levels, beta):
    pieces = [ref[...].astype(F32) for ref in refs]
    direct = sum(in_order(lax.axis_index("z"), pieces))
    applied = levels * vector - direct - beta * earlier
    square = chain_rows(vector * vector, s.chains)
    cross = chain_rows(vector * applied, s.chains)
    shift = jnp.where(square > 0.0, cross / jnp.where(square > 0.0, square, 1.0), 0.0)
    shift = shift.astype(BF).astype(F32)
    work = applied - shift * vector
    sums = (
        square,
        chain_rows(work * vector, s.chains),
        chain_rows(work * work, s.chains),
        shift,
    )
    lane = iota((s.rows, LANES), 1)
    value = jnp.zeros((s.rows, LANES), F32)
    for at, item in enumerate(sums):
        value = jnp.where(lane % 4 == at, item, value)
    high, middle, low = three_pieces(value)
    packed = jnp.where(lane < 4, high, jnp.where(lane < 8, middle, low))
    return work, packed


def read_sums(s, tiles):
    square, cross, work, shift = [], [], [], []
    for tile in tiles:
        value = tile[:, 0:4] + tile[:, 4:8] + tile[:, 8:12]
        for at, into in enumerate((square, cross, work, shift)):
            into.append(value[:, at : at + 1])
    alpha = sum(c + h * q for c, h, q in zip(cross, shift, square)) / s.entries
    offsets = [h - alpha for h in shift]
    mean = sum(
        w + 2.0 * o * c + o * (o * q) for w, o, c, q in zip(work, offsets, cross, square)
    )
    beta = jnp.sqrt(jnp.maximum(mean / s.entries, 0.0) + EPSILON)
    return alpha, beta, offsets


def later_kernel(s, *refs):
    direct_refs, refs = refs[: s.chips], refs[s.chips :]
    work_ref, vector_ref, levels_ref, scalars_ref, right_ref = refs[:5]
    packet_ref, new_work_ref, new_vector_ref = refs[5:]
    vector, beta = advance(work_ref, vector_ref, scalars_ref)
    new_vector_ref[...] = vector
    work, packed = apply_step(s, direct_refs, vector, vector_ref[...], levels_ref[...], beta)
    new_work_ref[...] = work
    finish_packet(s, work, packed, right_ref, packet_ref)


def first_kernel(s, *refs):
    direct_refs, refs = refs[: s.chips], refs[s.chips :]
    vector_ref, earlier_ref, levels_ref, beta_ref, right_ref = refs[:5]
    packet_ref, new_work_ref = refs[5:]
    beta = first_beta(s, beta_ref)
    work, packed = apply_step(
        s, direct_refs, vector_ref[...], earlier_ref[...], levels_ref[...], beta
    )
    new_work_ref[...] = work
    finish_packet(s, work, packed, right_ref, packet_ref)


def first_beta(s, beta_ref):
    row = iota((s.rows, 1), 0) // s.kpoints
    beta = jnp.zeros((s.rows, 1), F32)
    for n in range(s.chains):
        beta = jnp.where(row == n, beta_ref[:, n : n + 1], beta)
    return beta


def advance(work_ref, vector_ref, scalars_ref):
    beta = scalars_ref[:, 1:2]
    offset = scalars_ref[:, 2:3]
    return (work_ref[...] + offset * vector_ref[...]) / beta, beta


def finish_packet(s, work, packed, right_ref, packet_ref):
    send(s, project(s, high_low(work), right_ref), packed, packet_ref)


def last_kernel(s, *refs):
    direct_refs, refs = refs[: s.chips], refs[s.chips :]
    work_ref, vector_ref, levels_ref, scalars_ref = refs[:4]
    packet_ref, new_work_ref, new_vector_ref = refs[4:]
    vector, beta = advance(work_ref, vector_ref, scalars_ref)
    new_vector_ref[...] = vector
    work, packed = apply_step(s, direct_refs, vector, vector_ref[...], levels_ref[...], beta)
    new_work_ref[...] = work
    packet_ref[...] = packed


def in_order(me, pieces):
    ordered = []
    for source in range(len(pieces)):
        piece = pieces[0]
        for distance in range(1, len(pieces)):
            piece = jnp.where((me ^ source) == distance, pieces[distance], piece)
        ordered.append(piece)
    return ordered


def end_kernel(s, *refs):
    sums, refs = [ref[...] for ref in refs[: s.groups]], refs[s.groups :]
    work_ref, vector_ref = refs[:2]
    scalar_refs, targets, held, sems = refs[2:-9], refs[-9:-5], refs[-5:-1], refs[-1]
    last_ref, prior_ref, alphas_ref, betas_ref = held
    alpha, beta, offsets = read_sums(s, in_order(lax.axis_index("kpt"), sums))
    offset = own_offset(s, offsets)
    vector = vector_ref[...]
    last = (work_ref[...] + offset * vector) / beta
    width = last_ref.shape[2]
    me = lax.axis_index("z") * CORES + lax.axis_index("core")
    k = s.kpoints
    for value, ref in ((last, last_ref), (vector, prior_ref)):
        own = jnp.zeros((s.rows, width), F32)
        for b in range(s.parts):
            own = jnp.where(me == b, value[:, b * width : (b + 1) * width], own)
        for n in range(s.chains):
            ref[n] = own[n * k : (n + 1) * k]
    alphas = [ref[:, 0:1] for ref in scalar_refs] + [alpha]
    betas = [ref[:, 1:2] for ref in scalar_refs] + [beta]
    for n in range(s.chains):
        at = slice(n * k, n * k + 1)
        alphas_ref[n : n + 1, :] = jnp.concatenate([x[at] for x in alphas], axis=1)
        betas_ref[n : n + 1, :] = jnp.concatenate([x[at] for x in betas], axis=1)
    copy_all(held, targets, sems)


def own_offset(s, offsets):
    me = lax.axis_index("kpt")
    own = jnp.zeros_like(offsets[0])
    for a in range(s.groups):
        own = jnp.where(me == a, offsets[a], own)
    return own


def images(s, packet_ref, screened_ref, other):
    width = packet_ref.shape[2] - LANES
    rows, core = s.rows, lax.axis_index("core") ^ other
    columns = []
    for z in range(s.chips):
        blocks = [
            packet_ref[a * s.chips + z, :, :width].astype(F32) for a in range(s.groups)
        ]
        columns.append(jnp.concatenate(blocks, axis=0).astype(BF))
    result = []
    for q in range(s.transfers):
        image = None
        for z in range(s.chips):
            part = z * CORES + core
            lanes = pl.ds(pl.multiple_of(part * width, width), width)
            piece = lax.dot_general(
                screened_ref[q, :, lanes],
                columns[z],
                (((1,), (1,)), ((), ())),
                preferred_element_type=F32,
            )
            image = piece if image is None else image + piece
        result.append(image.T)
    return result


def half_kernel(s, packet_ref, screened_ref, image_ref):
    for q, image in enumerate(images(s, packet_ref, screened_ref, 0)):
        image_ref[q] = image


def screen_kernel(s, first, keep, *refs):
    refs = list(refs)
    half_ref = refs.pop(0)
    packet_refs = refs[:CORES]
    del refs[:CORES]
    before_ref = None if first else refs.pop(0)
    screened_ref, pick_ref = refs[:2]
    out_refs = refs[2 : 2 + s.groups]
    del refs[: 2 + s.groups]
    scalars_ref = None if first else refs.pop(0)
    image_ref = refs.pop(0) if keep else None
    (field_ref,) = refs
    rows = s.rows
    width = packet_refs[0].shape[2] - LANES
    core = lax.axis_index("core")
    if not first:
        tiles = [
            jnp.where(
                core == 0, *(ref[a * s.chips, :, width:].astype(F32) for ref in packet_refs)
            )
            for a in range(s.groups)
        ]
        alpha, beta, offsets = read_sums(s, tiles)
        scale = 1.0 / beta
        lane = iota((rows, LANES), 1)
        scalars_ref[...] = jnp.where(
            lane == 0, alpha, jnp.where(lane == 1, beta, own_offset(s, offsets))
        )
        shifts = jnp.concatenate(offsets, axis=0)
        scales = jnp.concatenate([scale] * s.groups, axis=0)
    pieces = []
    for q, image in enumerate(images(s, packet_refs[1], screened_ref, 1)):
        image = image + half_ref[q]
        if not first:
            image = (image + shifts * before_ref[q]) * scales
        if keep:
            image_ref[q] = image
        pieces.extend(three_pieces(image))
    stacked = jnp.concatenate([piece.astype(BF) for piece in pieces], axis=0)
    field_ref[...] = jnp.dot(pick_ref[...], stacked, preferred_element_type=F32)
    mine = lax.axis_index("kpt")
    for a in range(s.groups):
        out_refs[a][...] = field_ref[pl.ds(pl.multiple_of((mine ^ a) * rows, rows), rows), :]


def field_kernel(s, first, *refs):
    left_ref, out_ref = refs[-2:]
    field = refs[0][...]
    for ref in refs[1:-2]:
        field = field + ref[...]
    parts = (field.astype(BF),) if first else high_low(field)
    stacked = jnp.concatenate([p.astype(F32) for p in parts], axis=0).astype(BF)
    rows = s.rows
    direct = None
    for k in range(s.kpoints):
        image = lax.dot_general(
            stacked, left_ref[k], (((1,), (1,)), ((), ())), preferred_element_type=F32
        )
        if not first:
            image = image[:rows] + image[rows:]
        own = iota(image.shape, 0) % s.kpoints == k
        direct = jnp.where(own, image, 0.0 if direct is None else direct)
    out_ref[...] = direct


class Sizes:
    pass


VMEM = pl.BlockSpec(memory_space=pltpu.VMEM)
HBM = pl.BlockSpec(memory_space=pltpu.HBM)


def call(body, args, outs, name, specs=None, out_specs=None, scratch=(), limit=24, cost=0):
    return pl.pallas_call(
        body,
        out_shape=[jax.ShapeDtypeStruct(shape, dtype) for shape, dtype in outs],
        in_specs=specs or [VMEM] * len(args),
        out_specs=out_specs or [VMEM] * len(outs),
        scratch_shapes=list(scratch),
        compiler_params=pltpu.CompilerParams(vmem_limit_bytes=limit * 1024 * 1024),
        name=name,
        cost_estimate=pl.CostEstimate(
            flops=cost, bytes_accessed=cost // 256, transcendentals=0
        ),
    )(*args)


def on_device(
    groups, parts,
    energies, current, previous, previous_beta, pair_left, pair_right, screened, momentum_index
):
    s = Sizes()
    s.groups, s.parts, s.chips = groups, parts, parts // CORES
    s.chains, s.kpoints, band_block = current.shape
    s.rows = s.chains * s.kpoints
    s.transfers, width, waves = screened.shape
    bands = pair_left.shape[1]
    nk = momentum_index.shape[0]
    s.entries = float(nk * bands)
    total = groups * s.rows
    state = ((s.rows, bands), F32)
    packet = ((groups * parts // CORES, s.rows, width + LANES), BF)
    chip = ("z", "core")

    def exchange(x, axes):
        return lax.all_to_all(x, axes, 0, 0, tiled=True)

    def across(x, axis, size, distance):
        return lax.ppermute(x, axis, [(i, i ^ distance) for i in range(size)])

    def swap(pieces, axis="kpt"):
        return [pieces[0]] + [
            across(piece, axis, len(pieces), at) for at, piece in enumerate(pieces) if at
        ]

    screened = pltpu.with_memory_space_constraint(screened, pltpu.VMEM)
    inputs = tuple(
        pltpu.with_memory_space_constraint(x, pltpu.HBM)
        for x in (momentum_index, current, previous, energies)
    )
    pick, start = call(
        functools.partial(begin_kernel, s),
        inputs,
        [
            ((total, s.transfers * 3 * total), BF),
            ((parts, 2 * s.rows, 2 * band_block), F32),
        ],
        "begin",
        specs=[HBM] * len(inputs),
        scratch=[pltpu.VMEM(x.shape, x.dtype) for x in inputs]
        + [pltpu.SemaphoreType.DMA((len(inputs),))],
        cost=COVER,
    )
    start = exchange(start, chip)
    sent, vector, earlier, levels = call(
        functools.partial(unpack_kernel, s),
        (start, pair_right),
        [packet, state, state, state],
        "unpack",
        cost=COVER,
    )
    scalars = []
    before = work = None
    for step in range(STEPS):
        first, keep = step == 0, step < STEPS - 1
        got = exchange(sent, ("kpt", "z"))
        other = across(got, "core", CORES, 1)
        image = ((s.transfers, total, width), F32)
        (half,) = call(
            functools.partial(half_kernel, s), (got, screened), [image], "half", cost=COVER
        )
        args = (half, got, other) + (() if first else (before,)) + (screened, pick)
        outs = [((s.rows, width), F32)] * groups
        outs += [] if first else [((s.rows, LANES), F32)]
        outs += [image] if keep else []
        results = call(
            functools.partial(screen_kernel, s, first, keep),
            args,
            outs,
            "screen",
            scratch=[pltpu.VMEM((total, width), F32)],
        )
        if not first:
            scalars.append(results[groups])
        if keep:
            before = results[-1]
        (direct,) = call(
            functools.partial(field_kernel, s, first),
            (*swap(results[:groups]), pair_left),
            [state],
            "field",
        )
        (direct,) = call(
            functools.partial(pair_kernel, s),
            (direct, across(direct, "core", CORES, 1)),
            [((s.rows, bands), BF)],
            "pair",
        )
        direct = swap([direct] * s.chips, "z")
        if first:
            sent, work = call(
                functools.partial(first_kernel, s),
                (*direct, vector, earlier, levels, previous_beta[None], pair_right),
                [packet, state],
                "apply",
            )
        elif keep:
            sent, work, vector = call(
                functools.partial(later_kernel, s),
                (*direct, work, vector, levels, scalars[-1], pair_right),
                [packet, state, state],
                "apply",
            )
        else:
            sent, work, vector = call(
                functools.partial(last_kernel, s),
                (*direct, work, vector, levels, scalars[-1]),
                [((s.rows, LANES), F32), state, state],
                "apply",
            )
    sums = swap([sent] * groups)
    own = (current.shape, F32)
    terms = ((s.chains, STEPS), F32)
    return tuple(
        call(
            functools.partial(end_kernel, s),
            (*sums, work, vector, *scalars),
            [own, own, terms, terms],
            "end",
            out_specs=[HBM] * 4,
            scratch=[pltpu.VMEM(*x) for x in (own, own, terms, terms)]
            + [pltpu.SemaphoreType.DMA((4,))],
        )
    )


def solution(mesh):
    groups, parts = mesh.shape["kpt"], mesh.shape["pw"]
    devices = mesh.devices.reshape(groups, parts // CORES, CORES)
    pw = ("z", "core")
    return jax.shard_map(
        functools.partial(on_device, groups, parts),
        mesh=jax.sharding.Mesh(devices, ("kpt", *pw)),
        in_specs=(
            P("kpt", pw),
            P(None, "kpt", pw),
            P(None, "kpt", pw),
            P(),
            P("kpt", None, pw),
            P("kpt", None, pw),
            P("kpt", pw, None),
            P(),
        ),
        out_specs=(P(None, "kpt", pw), P(None, "kpt", pw), P(), P()),
        check_vma=False,
    )
```

```python
import functools

import jax
import jax.numpy as jnp
from jax import lax
from jax.experimental import pallas as pl
from jax.experimental.pallas import tpu as pltpu
from jax.sharding import PartitionSpec as P

STEPS = 3
EPSILON = 1e-06
COVER = 10_000_000_000
LANES = 128
CORES = 2
BF, F32 = jnp.bfloat16, jnp.float32


def iota(shape, axis):
    return lax.broadcasted_iota(jnp.int32, shape, axis)


def high_low(x):
    high = x.astype(BF)
    return high, (x - high.astype(F32)).astype(BF)


def three_pieces(x):
    high = x.astype(BF).astype(F32)
    rest = x - high
    middle = rest.astype(BF).astype(F32)
    return high, middle, (rest - middle).astype(BF).astype(F32)


def chain_rows(x, chains):
    rows = x.shape[0] // chains
    parts = []
    for n in range(chains):
        part = jnp.sum(x[n * rows : (n + 1) * rows], axis=(0, 1), keepdims=True)
        parts.append(jnp.broadcast_to(part, (rows, 1)))
    return jnp.concatenate(parts, axis=0)


def copy_all(sources, targets, sems):
    started = [
        pltpu.make_async_copy(source, target, sems.at[at])
        for at, (source, target) in enumerate(zip(sources, targets))
    ]
    for copy in started:
        copy.start()
    for copy in started:
        copy.wait()


def begin_kernel(s, *refs):
    sources, out_ref, held, sems = refs[:3], refs[3], refs[4:7], refs[7]
    copy_all(sources, held, sems)
    current_ref, previous_ref, energies_ref = held
    both = []
    for ref in (current_ref, previous_ref):
        both.append(jnp.concatenate([ref[n] for n in range(s.chains)], axis=0))
    levels = jnp.concatenate([energies_ref[...]] * s.chains, axis=0)
    out_ref[...] = jnp.concatenate(
        [jnp.concatenate(both, axis=1), jnp.concatenate([levels] * 2, axis=1)], axis=0
    )


def stack_kernel(s, own_ref, other_ref, out_ref):
    core = lax.axis_index("core")
    height = own_ref.shape[0]
    for c in range(CORES):
        value = jnp.where(core == c, own_ref[...], other_ref[...])
        out_ref[c * height : (c + 1) * height, :] = value


def pick_kernel(s, mi_ref, pick_ref):
    rows = s.rows
    mi = mi_ref[...].astype(F32).astype(BF)
    total, nk = s.groups * rows, mi.shape[0]

    def kpoint(r):
        return (r // rows) * s.kpoints + r % s.kpoints

    def chain(r):
        return (r % rows) // s.kpoints

    left = (kpoint(iota((total, nk), 0)) == iota((total, nk), 1)).astype(F32).astype(BF)
    right = (iota((nk, total), 0) == kpoint(iota((nk, total), 1))).astype(F32).astype(BF)
    spread = jnp.dot(left, mi, preferred_element_type=F32)
    spread = jnp.dot(spread.astype(BF), right, preferred_element_type=F32)
    same = chain(iota((total, total), 0)) == chain(iota((total, total), 1))
    for q in range(s.transfers):
        wanted = (lax.axis_index("kpt") * s.transfers + q).astype(F32)
        one = jnp.where(jnp.logical_and(spread == wanted, same), 1.0, 0.0).astype(BF)
        for piece in range(3):
            at = (q * 3 + piece) * total
            pick_ref[:, at : at + total] = one


def unpack_kernel(s, *refs):
    right_ref, _, packet_ref, vector_ref, earlier_ref, levels_ref = refs[s.chips :]
    rows = s.rows
    width = refs[0].shape[1] // 2
    pieces = in_order(lax.axis_index("z"), [ref[...] for ref in refs[: s.chips]])
    for ref, row, lane in ((vector_ref, 0, 0), (earlier_ref, 0, width), (levels_ref, rows, 0)):
        blocks = []
        for piece in pieces:
            for c in range(CORES):
                at = 2 * rows * c + row
                blocks.append(piece[at : at + rows, lane : lane + width])
        ref[...] = jnp.concatenate(blocks, axis=1)
    density = project(s, (vector_ref[...].astype(BF),), right_ref)
    send(s, density, jnp.zeros((rows, LANES), F32), packet_ref)


def project(s, parts, right_ref):
    x = jnp.concatenate([part.astype(F32) for part in parts], axis=0)
    total = None
    for k in range(s.kpoints):
        own = iota(x.shape, 0) % s.kpoints == k
        masked = jnp.where(own, x, 0.0).astype(BF)
        part = jnp.dot(masked, right_ref[k], preferred_element_type=F32)
        total = part if total is None else total + part
    return sum(total[at : at + s.rows] for at in range(0, x.shape[0], s.rows))


def send(s, density, sums, packet_ref):
    width = density.shape[1]
    density = density.astype(BF)
    sums = sums.astype(BF)
    for d in range(packet_ref.shape[0]):
        packet_ref[d, :, :width] = density
        packet_ref[d, :, width:] = sums


def pair_kernel(s, own_ref, other_ref, out_ref):
    out_ref[...] = (own_ref[...] + other_ref[...]).astype(BF)


def apply_step(s, refs, vector, earlier, levels, beta):
    pieces = [ref[...].astype(F32) for ref in refs]
    direct = sum(in_order(lax.axis_index("z"), pieces))
    applied = levels * vector - direct - beta * earlier
    square = chain_rows(vector * vector, s.chains)
    cross = chain_rows(vector * applied, s.chains)
    shift = jnp.where(square > 0.0, cross / jnp.where(square > 0.0, square, 1.0), 0.0)
    shift = shift.astype(BF).astype(F32)
    work = applied - shift * vector
    sums = (
        square,
        chain_rows(work * vector, s.chains),
        chain_rows(work * work, s.chains),
        shift,
    )
    lane = iota((s.rows, LANES), 1)
    value = jnp.zeros((s.rows, LANES), F32)
    for at, item in enumerate(sums):
        value = jnp.where(lane % 4 == at, item, value)
    high, middle, low = three_pieces(value)
    packed = jnp.where(lane < 4, high, jnp.where(lane < 8, middle, low))
    return work, packed


def read_sums(s, tiles):
    square, cross, work, shift = [], [], [], []
    for tile in tiles:
        value = tile[:, 0:4] + tile[:, 4:8] + tile[:, 8:12]
        for at, into in enumerate((square, cross, work, shift)):
            into.append(value[:, at : at + 1])
    alpha = sum(c + h * q for c, h, q in zip(cross, shift, square)) / s.entries
    offsets = [h - alpha for h in shift]
    mean = sum(
        w + 2.0 * o * c + o * (o * q) for w, o, c, q in zip(work, offsets, cross, square)
    )
    beta = jnp.sqrt(jnp.maximum(mean / s.entries, 0.0) + EPSILON)
    return alpha, beta, offsets


def later_kernel(s, *refs):
    direct_refs, refs = refs[: s.chips], refs[s.chips :]
    work_ref, vector_ref, levels_ref, scalars_ref, right_ref = refs[:5]
    packet_ref, new_work_ref, new_vector_ref = refs[5:]
    vector, beta = advance(work_ref, vector_ref, scalars_ref)
    new_vector_ref[...] = vector
    work, packed = apply_step(s, direct_refs, vector, vector_ref[...], levels_ref[...], beta)
    new_work_ref[...] = work
    finish_packet(s, work, packed, right_ref, packet_ref)


def first_kernel(s, *refs):
    direct_refs, refs = refs[: s.chips], refs[s.chips :]
    vector_ref, earlier_ref, levels_ref, beta_ref, right_ref = refs[:5]
    packet_ref, new_work_ref = refs[5:]
    beta = first_beta(s, beta_ref)
    work, packed = apply_step(
        s, direct_refs, vector_ref[...], earlier_ref[...], levels_ref[...], beta
    )
    new_work_ref[...] = work
    finish_packet(s, work, packed, right_ref, packet_ref)


def first_beta(s, beta_ref):
    row = iota((s.rows, 1), 0) // s.kpoints
    beta = jnp.zeros((s.rows, 1), F32)
    for n in range(s.chains):
        beta = jnp.where(row == n, beta_ref[:, n : n + 1], beta)
    return beta


def advance(work_ref, vector_ref, scalars_ref):
    beta = scalars_ref[:, 1:2]
    offset = scalars_ref[:, 2:3]
    return (work_ref[...] + offset * vector_ref[...]) / beta, beta


def finish_packet(s, work, packed, right_ref, packet_ref):
    send(s, project(s, high_low(work), right_ref), packed, packet_ref)


def last_kernel(s, *refs):
    direct_refs, refs = refs[: s.chips], refs[s.chips :]
    work_ref, vector_ref, levels_ref, scalars_ref = refs[:4]
    packet_ref, new_work_ref, new_vector_ref = refs[4:]
    vector, beta = advance(work_ref, vector_ref, scalars_ref)
    new_vector_ref[...] = vector
    work, packed = apply_step(s, direct_refs, vector, vector_ref[...], levels_ref[...], beta)
    new_work_ref[...] = work
    packet_ref[...] = packed


def in_order(me, pieces):
    ordered = []
    for source in range(len(pieces)):
        piece = pieces[0]
        for distance in range(1, len(pieces)):
            piece = jnp.where((me ^ source) == distance, pieces[distance], piece)
        ordered.append(piece)
    return ordered


def own_kernel(s, work_ref, vector_ref, *refs):
    scalar_refs = refs[:-6]
    own_work_ref, own_vector_ref, terms_ref, prior_ref, prior, sem = refs[-6:]
    width = own_work_ref.shape[1]
    me = lax.axis_index("z") * CORES + lax.axis_index("core")
    for source, target in ((work_ref, own_work_ref), (vector_ref, own_vector_ref)):
        own = source[:, :width]
        for b in range(1, s.parts):
            own = jnp.where(me == b, source[:, b * width : (b + 1) * width], own)
        target[...] = own
    for n in range(s.chains):
        prior[n] = own_vector_ref[n * s.kpoints : (n + 1) * s.kpoints, :]
    copy = pltpu.make_async_copy(prior, prior_ref, sem.at[0])
    copy.start()
    lane = iota((s.rows, LANES), 1)
    terms = jnp.zeros((s.rows, LANES), F32)
    for at, ref in enumerate(scalar_refs):
        terms = jnp.where(lane == at, ref[:, 0:1], terms)
        terms = jnp.where(lane == STEPS + at, ref[:, 1:2], terms)
    terms_ref[...] = terms
    copy.wait()


def end_kernel(s, *refs):
    sums, refs = [ref[...] for ref in refs[: s.groups]], refs[s.groups :]
    work_ref, vector_ref, terms_ref = refs[:3]
    targets, held, sems = refs[3:6], refs[6:9], refs[9]
    last_ref, alphas_ref, betas_ref = held
    alpha, beta, offsets = read_sums(s, in_order(lax.axis_index("kpt"), sums))
    offset = own_offset(s, offsets)
    last = (work_ref[...] + offset * vector_ref[...]) / beta
    lane = iota((s.rows, LANES), 1)
    terms = jnp.where(lane == STEPS - 1, alpha, terms_ref[...])
    terms = jnp.where(lane == 2 * STEPS - 1, beta, terms)
    k = s.kpoints
    for n in range(s.chains):
        last_ref[n] = last[n * k : (n + 1) * k]
        alphas_ref[n : n + 1, :] = terms[n * k : n * k + 1, :STEPS]
        betas_ref[n : n + 1, :] = terms[n * k : n * k + 1, STEPS : 2 * STEPS]
    copy_all(held, targets, sems)


def own_offset(s, offsets):
    me = lax.axis_index("kpt")
    own = jnp.zeros_like(offsets[0])
    for a in range(s.groups):
        own = jnp.where(me == a, offsets[a], own)
    return own


def images(s, packet_ref, screened_ref, other):
    width = packet_ref.shape[2] - LANES
    rows, core = s.rows, lax.axis_index("core") ^ other
    columns = []
    for z in range(s.chips):
        blocks = [
            packet_ref[a * s.chips + z, :, :width].astype(F32) for a in range(s.groups)
        ]
        columns.append(jnp.concatenate(blocks, axis=0).astype(BF))
    result = []
    for q in range(s.transfers):
        image = None
        for z in range(s.chips):
            part = z * CORES + core
            lanes = pl.ds(pl.multiple_of(part * width, width), width)
            piece = lax.dot_general(
                screened_ref[q, :, lanes],
                columns[z],
                (((1,), (1,)), ((), ())),
                preferred_element_type=F32,
            )
            image = piece if image is None else image + piece
        result.append(image.T)
    return result


def half_kernel(s, packet_ref, screened_ref, image_ref):
    for q, image in enumerate(images(s, packet_ref, screened_ref, 0)):
        image_ref[q] = image


def screen_kernel(s, first, keep, *refs):
    refs = list(refs)
    half_ref = refs.pop(0)
    packet_refs = refs[:CORES]
    del refs[:CORES]
    before_ref = None if first else refs.pop(0)
    screened_ref, pick_ref = refs[:2]
    out_refs = refs[2 : 2 + s.groups]
    del refs[: 2 + s.groups]
    scalars_ref = None if first else refs.pop(0)
    image_ref = refs.pop(0) if keep else None
    (field_ref,) = refs
    rows = s.rows
    width = packet_refs[0].shape[2] - LANES
    core = lax.axis_index("core")
    if not first:
        tiles = [
            jnp.where(
                core == 0, *(ref[a * s.chips, :, width:].astype(F32) for ref in packet_refs)
            )
            for a in range(s.groups)
        ]
        alpha, beta, offsets = read_sums(s, tiles)
        scale = 1.0 / beta
        lane = iota((rows, LANES), 1)
        scalars_ref[...] = jnp.where(
            lane == 0, alpha, jnp.where(lane == 1, beta, own_offset(s, offsets))
        )
        shifts = jnp.concatenate(offsets, axis=0)
        scales = jnp.concatenate([scale] * s.groups, axis=0)
    pieces = []
    for q, image in enumerate(images(s, packet_refs[1], screened_ref, 1)):
        image = image + half_ref[q]
        if not first:
            image = (image + shifts * before_ref[q]) * scales
        if keep:
            image_ref[q] = image
        pieces.extend(three_pieces(image))
    stacked = jnp.concatenate([piece.astype(BF) for piece in pieces], axis=0)
    field_ref[...] = jnp.dot(pick_ref[...], stacked, preferred_element_type=F32)
    mine = lax.axis_index("kpt")
    for a in range(s.groups):
        out_refs[a][...] = field_ref[pl.ds(pl.multiple_of((mine ^ a) * rows, rows), rows), :]


def field_kernel(s, first, *refs):
    left_ref, out_ref = refs[-2:]
    field = refs[0][...]
    for ref in refs[1:-2]:
        field = field + ref[...]
    parts = (field.astype(BF),) if first else high_low(field)
    stacked = jnp.concatenate([p.astype(F32) for p in parts], axis=0).astype(BF)
    rows = s.rows
    direct = None
    for k in range(s.kpoints):
        image = lax.dot_general(
            stacked, left_ref[k], (((1,), (1,)), ((), ())), preferred_element_type=F32
        )
        if not first:
            image = image[:rows] + image[rows:]
        own = iota(image.shape, 0) % s.kpoints == k
        direct = jnp.where(own, image, 0.0 if direct is None else direct)
    out_ref[...] = direct


class Sizes:
    pass


VMEM = pl.BlockSpec(memory_space=pltpu.VMEM)
HBM = pl.BlockSpec(memory_space=pltpu.HBM)


def call(body, args, outs, name, specs=None, out_specs=None, scratch=(), limit=24, cost=0):
    return pl.pallas_call(
        body,
        out_shape=[jax.ShapeDtypeStruct(shape, dtype) for shape, dtype in outs],
        in_specs=specs or [VMEM] * len(args),
        out_specs=out_specs or [VMEM] * len(outs),
        scratch_shapes=list(scratch),
        compiler_params=pltpu.CompilerParams(vmem_limit_bytes=limit * 1024 * 1024),
        name=name,
        cost_estimate=pl.CostEstimate(
            flops=cost, bytes_accessed=cost // 256, transcendentals=0
        ),
    )(*args)


def on_device(
    groups, parts,
    energies, current, previous, previous_beta, pair_left, pair_right, screened, momentum_index
):
    s = Sizes()
    s.groups, s.parts, s.chips = groups, parts, parts // CORES
    s.chains, s.kpoints, band_block = current.shape
    s.rows = s.chains * s.kpoints
    s.transfers, width, waves = screened.shape
    bands = pair_left.shape[1]
    nk = momentum_index.shape[0]
    s.entries = float(nk * bands)
    total = groups * s.rows
    state = ((s.rows, bands), F32)
    packet = ((groups * parts // CORES, s.rows, width + LANES), BF)

    def exchange(x, axes):
        return lax.all_to_all(x, axes, 0, 0, tiled=True)

    def across(x, axis, size, distance):
        return lax.ppermute(x, axis, [(i, i ^ distance) for i in range(size)])

    def swap(pieces, axis="kpt"):
        return [pieces[0]] + [
            across(piece, axis, len(pieces), at) for at, piece in enumerate(pieces) if at
        ]

    screened = pltpu.with_memory_space_constraint(screened, pltpu.VMEM)
    inputs = tuple(
        pltpu.with_memory_space_constraint(x, pltpu.HBM)
        for x in (current, previous, energies)
    )
    piece = ((2 * s.rows, 2 * band_block), F32)
    (start,) = call(
        functools.partial(begin_kernel, s),
        inputs,
        [piece],
        "begin",
        specs=[HBM] * len(inputs),
        scratch=[pltpu.VMEM(x.shape, x.dtype) for x in inputs]
        + [pltpu.SemaphoreType.DMA((len(inputs),))],
        cost=COVER,
    )
    (start,) = call(
        functools.partial(stack_kernel, s),
        (start, across(start, "core", CORES, 1)),
        [((CORES * 2 * s.rows, 2 * band_block), F32)],
        "stack",
    )
    (pick,) = call(
        functools.partial(pick_kernel, s),
        (momentum_index,),
        [((total, s.transfers * 3 * total), BF)],
        "pick",
    )
    start = swap([start] * s.chips, "z")
    sent, vector, earlier, levels = call(
        functools.partial(unpack_kernel, s),
        (*start, pair_right, pick),
        [packet, state, state, state],
        "unpack",
        cost=COVER,
    )
    scalars = []
    before = work = None
    for step in range(STEPS):
        first, keep = step == 0, step < STEPS - 1
        got = exchange(sent, ("kpt", "z"))
        other = across(got, "core", CORES, 1)
        image = ((s.transfers, total, width), F32)
        (half,) = call(
            functools.partial(half_kernel, s), (got, screened), [image], "half", cost=COVER
        )
        args = (half, got, other) + (() if first else (before,)) + (screened, pick)
        outs = [((s.rows, width), F32)] * groups
        outs += [] if first else [((s.rows, LANES), F32)]
        outs += [image] if keep else []
        results = call(
            functools.partial(screen_kernel, s, first, keep),
            args,
            outs,
            "screen",
            scratch=[pltpu.VMEM((total, width), F32)],
        )
        if not first:
            scalars.append(results[groups])
        if keep:
            before = results[-1]
        (direct,) = call(
            functools.partial(field_kernel, s, first),
            (*swap(results[:groups])[::-1], pair_left),
            [state],
            "field",
        )
        (direct,) = call(
            functools.partial(pair_kernel, s),
            (direct, across(direct, "core", CORES, 1)),
            [((s.rows, bands), BF)],
            "pair",
        )
        direct = swap([direct] * s.chips, "z")
        if first:
            sent, work = call(
                functools.partial(first_kernel, s),
                (*direct, vector, earlier, levels, previous_beta[None], pair_right),
                [packet, state],
                "apply",
            )
        elif keep:
            sent, work, vector = call(
                functools.partial(later_kernel, s),
                (*direct, work, vector, levels, scalars[-1], pair_right),
                [packet, state, state],
                "apply",
            )
        else:
            sent, work, vector = call(
                functools.partial(last_kernel, s),
                (*direct, work, vector, levels, scalars[-1]),
                [((s.rows, LANES), F32), state, state],
                "apply",
            )
    sums = swap([sent] * groups)
    own = (current.shape, F32)
    terms = ((s.chains, STEPS), F32)
    block = ((s.rows, band_block), F32)
    own_work, own_vector, known, prior = call(
        functools.partial(own_kernel, s),
        (work, vector, *scalars),
        [block, block, ((s.rows, LANES), F32), own],
        "own",
        out_specs=[VMEM] * 3 + [HBM],
        scratch=[pltpu.VMEM(*own), pltpu.SemaphoreType.DMA((1,))],
    )
    last, alphas, betas = call(
        functools.partial(end_kernel, s),
        (*sums, own_work, own_vector, known),
        [own, terms, terms],
        "end",
        out_specs=[HBM] * 3,
        scratch=[pltpu.VMEM(*x) for x in (own, terms, terms)]
        + [pltpu.SemaphoreType.DMA((3,))],
    )
    return last, prior, alphas, betas


def solution(mesh):
    groups, parts = mesh.shape["kpt"], mesh.shape["pw"]
    devices = mesh.devices.reshape(groups, parts // CORES, CORES)
    pw = ("z", "core")
    return jax.shard_map(
        functools.partial(on_device, groups, parts),
        mesh=jax.sharding.Mesh(devices, ("kpt", *pw)),
        in_specs=(
            P("kpt", pw),
            P(None, "kpt", pw),
            P(None, "kpt", pw),
            P(),
            P("kpt", None, pw),
            P("kpt", None, pw),
            P("kpt", pw, None),
            P(),
        ),
        out_specs=(P(None, "kpt", pw), P(None, "kpt", pw), P(), P()),
        check_vma=False,
    )
```

```python
import functools

import jax
import jax.numpy as jnp
from jax import lax
from jax.experimental import pallas as pl
from jax.experimental.pallas import tpu as pltpu
from jax.sharding import PartitionSpec as P

STEPS = 3
EPSILON = 1e-06
COVER = 10_000_000_000
LANES = 128
CORES = 2
BF, F32 = jnp.bfloat16, jnp.float32


def iota(shape, axis):
    return lax.broadcasted_iota(jnp.int32, shape, axis)


def high_low(x):
    high = x.astype(BF)
    return high, (x - high.astype(F32)).astype(BF)


def three_pieces(x):
    high = x.astype(BF).astype(F32)
    rest = x - high
    middle = rest.astype(BF).astype(F32)
    return high, middle, (rest - middle).astype(BF).astype(F32)


def chain_rows(x, chains):
    rows = x.shape[0] // chains
    parts = []
    for n in range(chains):
        part = jnp.sum(x[n * rows : (n + 1) * rows], axis=(0, 1), keepdims=True)
        parts.append(jnp.broadcast_to(part, (rows, 1)))
    return jnp.concatenate(parts, axis=0)


def copy_all(sources, targets, sems):
    started = [
        pltpu.make_async_copy(source, target, sems.at[at])
        for at, (source, target) in enumerate(zip(sources, targets))
    ]
    for copy in started:
        copy.start()
    for copy in started:
        copy.wait()


def begin_kernel(s, *refs):
    sources, out_ref, held, sems = refs[:3], refs[3], refs[4:7], refs[7]
    copy_all(sources, held, sems)
    current_ref, previous_ref, energies_ref = held
    both = []
    for ref in (current_ref, previous_ref):
        both.append(jnp.concatenate([ref[n] for n in range(s.chains)], axis=0))
    levels = jnp.concatenate([energies_ref[...]] * s.chains, axis=0)
    out_ref[...] = jnp.concatenate(
        [jnp.concatenate(both, axis=1), jnp.concatenate([levels] * 2, axis=1)], axis=0
    )


def stack_kernel(s, own_ref, other_ref, out_ref):
    core = lax.axis_index("core")
    height = own_ref.shape[0]
    for c in range(CORES):
        value = jnp.where(core == c, own_ref[...], other_ref[...])
        out_ref[c * height : (c + 1) * height, :] = value


def pick_kernel(s, mi_ref, pick_ref):
    rows = s.rows
    mi = mi_ref[...].astype(F32).astype(BF)
    total, nk = s.groups * rows, mi.shape[0]

    def kpoint(r):
        return (r // rows) * s.kpoints + r % s.kpoints

    def chain(r):
        return (r % rows) // s.kpoints

    left = (kpoint(iota((total, nk), 0)) == iota((total, nk), 1)).astype(F32).astype(BF)
    right = (iota((nk, total), 0) == kpoint(iota((nk, total), 1))).astype(F32).astype(BF)
    spread = jnp.dot(left, mi, preferred_element_type=F32)
    spread = jnp.dot(spread.astype(BF), right, preferred_element_type=F32)
    same = chain(iota((total, total), 0)) == chain(iota((total, total), 1))
    for q in range(s.transfers):
        wanted = (lax.axis_index("kpt") * s.transfers + q).astype(F32)
        one = jnp.where(jnp.logical_and(spread == wanted, same), 1.0, 0.0).astype(BF)
        for piece in range(3):
            at = (q * 3 + piece) * total
            pick_ref[:, at : at + total] = one


def unpack_kernel(s, *refs):
    right_ref, _, packet_ref, vector_ref, earlier_ref, levels_ref = refs[s.chips :]
    rows = s.rows
    width = refs[0].shape[1] // 2
    pieces = in_order(lax.axis_index("z"), [ref[...] for ref in refs[: s.chips]])
    for ref, row, lane in ((vector_ref, 0, 0), (earlier_ref, 0, width), (levels_ref, rows, 0)):
        blocks = []
        for piece in pieces:
            for c in range(CORES):
                at = 2 * rows * c + row
                blocks.append(piece[at : at + rows, lane : lane + width])
        ref[...] = jnp.concatenate(blocks, axis=1)
    density = project(s, (vector_ref[...].astype(BF),), right_ref)
    send(s, density, jnp.zeros((rows, LANES), F32), packet_ref)


def project(s, parts, right_ref):
    x = jnp.concatenate([part.astype(F32) for part in parts], axis=0)
    total = None
    for k in range(s.kpoints):
        own = iota(x.shape, 0) % s.kpoints == k
        masked = jnp.where(own, x, 0.0).astype(BF)
        part = jnp.dot(masked, right_ref[k], preferred_element_type=F32)
        total = part if total is None else total + part
    return sum(total[at : at + s.rows] for at in range(0, x.shape[0], s.rows))


def send(s, density, sums, packet_ref):
    half = density.shape[1] // CORES
    k = s.kpoints
    ends = [sums[n * k : n * k + 1] for n in range(s.chains)]
    for c in range(CORES):
        blocks = [density[:, at : at + LANES] for at in range(c * half, (c + 1) * half, LANES)]
        value = jnp.concatenate(blocks + ends, axis=0).astype(BF)
        value = value.reshape(packet_ref.shape[1:])
        for d in range(c, packet_ref.shape[0], CORES):
            packet_ref[d] = value


def received(s, packet_ref, d):
    value = packet_ref[d].reshape(-1, LANES).astype(F32)
    height = value.shape[0] - s.chains
    blocks = [value[at : at + s.rows] for at in range(0, height, s.rows)]
    sums = [
        jnp.broadcast_to(value[height + n : height + n + 1], (s.kpoints, LANES))
        for n in range(s.chains)
    ]
    return jnp.concatenate(blocks, axis=1), jnp.concatenate(sums, axis=0)


def pair_kernel(s, own_ref, other_ref, out_ref):
    out_ref[...] = (own_ref[...] + other_ref[...]).astype(BF)


def apply_step(s, refs, vector, earlier, levels, beta):
    pieces = [ref[...].astype(F32) for ref in refs]
    direct = sum(in_order(lax.axis_index("z"), pieces))
    applied = levels * vector - direct - beta * earlier
    square = chain_rows(vector * vector, s.chains)
    cross = chain_rows(vector * applied, s.chains)
    shift = jnp.where(square > 0.0, cross / jnp.where(square > 0.0, square, 1.0), 0.0)
    shift = shift.astype(BF).astype(F32)
    work = applied - shift * vector
    sums = (
        square,
        chain_rows(work * vector, s.chains),
        chain_rows(work * work, s.chains),
        shift,
    )
    lane = iota((s.rows, LANES), 1)
    value = jnp.zeros((s.rows, LANES), F32)
    for at, item in enumerate(sums):
        value = jnp.where(lane % 4 == at, item, value)
    high, middle, low = three_pieces(value)
    packed = jnp.where(lane < 4, high, jnp.where(lane < 8, middle, low))
    return work, packed


def read_sums(s, tiles):
    square, cross, work, shift = [], [], [], []
    for tile in tiles:
        value = tile[:, 0:4] + tile[:, 4:8] + tile[:, 8:12]
        for at, into in enumerate((square, cross, work, shift)):
            into.append(value[:, at : at + 1])
    alpha = sum(c + h * q for c, h, q in zip(cross, shift, square)) / s.entries
    offsets = [h - alpha for h in shift]
    mean = sum(
        w + 2.0 * o * c + o * (o * q) for w, o, c, q in zip(work, offsets, cross, square)
    )
    beta = jnp.sqrt(jnp.maximum(mean / s.entries, 0.0) + EPSILON)
    return alpha, beta, offsets


def later_kernel(s, *refs):
    direct_refs, refs = refs[: s.chips], refs[s.chips :]
    work_ref, vector_ref, levels_ref, scalars_ref, right_ref = refs[:5]
    packet_ref, new_work_ref, new_vector_ref = refs[5:]
    vector, beta = advance(work_ref, vector_ref, scalars_ref)
    new_vector_ref[...] = vector
    work, packed = apply_step(s, direct_refs, vector, vector_ref[...], levels_ref[...], beta)
    new_work_ref[...] = work
    finish_packet(s, work, packed, right_ref, packet_ref)


def first_kernel(s, *refs):
    direct_refs, refs = refs[: s.chips], refs[s.chips :]
    vector_ref, earlier_ref, levels_ref, beta_ref, right_ref = refs[:5]
    packet_ref, new_work_ref = refs[5:]
    beta = first_beta(s, beta_ref)
    work, packed = apply_step(
        s, direct_refs, vector_ref[...], earlier_ref[...], levels_ref[...], beta
    )
    new_work_ref[...] = work
    finish_packet(s, work, packed, right_ref, packet_ref)


def first_beta(s, beta_ref):
    row = iota((s.rows, 1), 0) // s.kpoints
    beta = jnp.zeros((s.rows, 1), F32)
    for n in range(s.chains):
        beta = jnp.where(row == n, beta_ref[:, n : n + 1], beta)
    return beta


def advance(work_ref, vector_ref, scalars_ref):
    beta = scalars_ref[:, 1:2]
    offset = scalars_ref[:, 2:3]
    return (work_ref[...] + offset * vector_ref[...]) / beta, beta


def finish_packet(s, work, packed, right_ref, packet_ref):
    send(s, project(s, high_low(work), right_ref), packed, packet_ref)


def last_kernel(s, *refs):
    direct_refs, refs = refs[: s.chips], refs[s.chips :]
    work_ref, vector_ref, levels_ref, scalars_ref = refs[:4]
    packet_ref, new_work_ref, new_vector_ref = refs[4:]
    vector, beta = advance(work_ref, vector_ref, scalars_ref)
    new_vector_ref[...] = vector
    work, packed = apply_step(s, direct_refs, vector, vector_ref[...], levels_ref[...], beta)
    new_work_ref[...] = work
    packet_ref[...] = packed


def in_order(me, pieces):
    ordered = []
    for source in range(len(pieces)):
        piece = pieces[0]
        for distance in range(1, len(pieces)):
            piece = jnp.where((me ^ source) == distance, pieces[distance], piece)
        ordered.append(piece)
    return ordered


def own_kernel(s, work_ref, vector_ref, *refs):
    scalar_refs = refs[:-6]
    own_work_ref, own_vector_ref, terms_ref, prior_ref, prior, sem = refs[-6:]
    width = own_work_ref.shape[1]
    me = lax.axis_index("z") * CORES + lax.axis_index("core")
    for source, target in ((work_ref, own_work_ref), (vector_ref, own_vector_ref)):
        own = source[:, :width]
        for b in range(1, s.parts):
            own = jnp.where(me == b, source[:, b * width : (b + 1) * width], own)
        target[...] = own
    for n in range(s.chains):
        prior[n] = own_vector_ref[n * s.kpoints : (n + 1) * s.kpoints, :]
    copy = pltpu.make_async_copy(prior, prior_ref, sem.at[0])
    copy.start()
    lane = iota((s.rows, LANES), 1)
    terms = jnp.zeros((s.rows, LANES), F32)
    for at, ref in enumerate(scalar_refs):
        terms = jnp.where(lane == at, ref[:, 0:1], terms)
        terms = jnp.where(lane == STEPS + at, ref[:, 1:2], terms)
    terms_ref[...] = terms
    copy.wait()


def end_kernel(s, *refs):
    sums, refs = [ref[...] for ref in refs[: s.groups]], refs[s.groups :]
    work_ref, vector_ref, terms_ref = refs[:3]
    targets, held, sems = refs[3:6], refs[6:9], refs[9]
    last_ref, alphas_ref, betas_ref = held
    alpha, beta, offsets = read_sums(s, in_order(lax.axis_index("kpt"), sums))
    offset = own_offset(s, offsets)
    last = (work_ref[...] + offset * vector_ref[...]) / beta
    lane = iota((s.rows, LANES), 1)
    terms = jnp.where(lane == STEPS - 1, alpha, terms_ref[...])
    terms = jnp.where(lane == 2 * STEPS - 1, beta, terms)
    k = s.kpoints
    for n in range(s.chains):
        last_ref[n] = last[n * k : (n + 1) * k]
        alphas_ref[n : n + 1, :] = terms[n * k : n * k + 1, :STEPS]
        betas_ref[n : n + 1, :] = terms[n * k : n * k + 1, STEPS : 2 * STEPS]
    copy_all(held, targets, sems)


def own_offset(s, offsets):
    me = lax.axis_index("kpt")
    own = jnp.zeros_like(offsets[0])
    for a in range(s.groups):
        own = jnp.where(me == a, offsets[a], own)
    return own


def images(s, packet_ref, screened_ref, other):
    columns = []
    for b in range(s.parts):
        blocks = [received(s, packet_ref, a * s.parts + b)[0] for a in range(s.groups)]
        columns.append(jnp.concatenate(blocks, axis=0).astype(BF))
    half = columns[0].shape[1]
    core = lax.axis_index("core") ^ other
    result = []
    for q in range(s.transfers):
        image = None
        for b in range(s.parts):
            at = (b * CORES + core) * half
            piece = lax.dot_general(
                screened_ref[q, :, pl.ds(pl.multiple_of(at, half), half)],
                columns[b],
                (((1,), (1,)), ((), ())),
                preferred_element_type=F32,
            )
            image = piece if image is None else image + piece
        result.append(image.T)
    return result


def half_kernel(s, packet_ref, screened_ref, image_ref):
    for q, image in enumerate(images(s, packet_ref, screened_ref, 0)):
        image_ref[q] = image


def screen_kernel(s, first, keep, *refs):
    refs = list(refs)
    half_ref = refs.pop(0)
    packet_refs = refs[:CORES]
    del refs[:CORES]
    before_ref = None if first else refs.pop(0)
    screened_ref, pick_ref = refs[:2]
    out_refs = refs[2 : 2 + s.groups]
    del refs[: 2 + s.groups]
    scalars_ref = None if first else refs.pop(0)
    image_ref = refs.pop(0) if keep else None
    (field_ref,) = refs
    rows = s.rows
    if not first:
        tiles = [received(s, packet_refs[0], a * s.parts)[1] for a in range(s.groups)]
        alpha, beta, offsets = read_sums(s, tiles)
        scale = 1.0 / beta
        lane = iota((rows, LANES), 1)
        scalars_ref[...] = jnp.where(
            lane == 0, alpha, jnp.where(lane == 1, beta, own_offset(s, offsets))
        )
        shifts = jnp.concatenate(offsets, axis=0)
        scales = jnp.concatenate([scale] * s.groups, axis=0)
    pieces = []
    for q, image in enumerate(images(s, packet_refs[1], screened_ref, 1)):
        image = image + half_ref[q]
        if not first:
            image = (image + shifts * before_ref[q]) * scales
        if keep:
            image_ref[q] = image
        pieces.extend(three_pieces(image))
    stacked = jnp.concatenate([piece.astype(BF) for piece in pieces], axis=0)
    field_ref[...] = jnp.dot(pick_ref[...], stacked, preferred_element_type=F32)
    mine = lax.axis_index("kpt")
    for a in range(s.groups):
        out_refs[a][...] = field_ref[pl.ds(pl.multiple_of((mine ^ a) * rows, rows), rows), :]


def field_kernel(s, first, *refs):
    left_ref, out_ref = refs[-2:]
    field = refs[0][...]
    for ref in refs[1:-2]:
        field = field + ref[...]
    parts = (field.astype(BF),) if first else high_low(field)
    stacked = jnp.concatenate([p.astype(F32) for p in parts], axis=0).astype(BF)
    rows = s.rows
    direct = None
    for k in range(s.kpoints):
        image = lax.dot_general(
            stacked, left_ref[k], (((1,), (1,)), ((), ())), preferred_element_type=F32
        )
        if not first:
            image = image[:rows] + image[rows:]
        own = iota(image.shape, 0) % s.kpoints == k
        direct = jnp.where(own, image, 0.0 if direct is None else direct)
    out_ref[...] = direct


class Sizes:
    pass


VMEM = pl.BlockSpec(memory_space=pltpu.VMEM)
HBM = pl.BlockSpec(memory_space=pltpu.HBM)


def call(body, args, outs, name, specs=None, out_specs=None, scratch=(), limit=24, cost=0):
    return pl.pallas_call(
        body,
        out_shape=[jax.ShapeDtypeStruct(shape, dtype) for shape, dtype in outs],
        in_specs=specs or [VMEM] * len(args),
        out_specs=out_specs or [VMEM] * len(outs),
        scratch_shapes=list(scratch),
        compiler_params=pltpu.CompilerParams(vmem_limit_bytes=limit * 1024 * 1024),
        name=name,
        cost_estimate=pl.CostEstimate(
            flops=cost, bytes_accessed=cost // 256, transcendentals=0
        ),
    )(*args)


def on_device(
    groups, parts,
    energies, current, previous, previous_beta, pair_left, pair_right, screened, momentum_index
):
    s = Sizes()
    s.groups, s.parts, s.chips = groups, parts, parts // CORES
    s.chains, s.kpoints, band_block = current.shape
    s.rows = s.chains * s.kpoints
    s.transfers, width, waves = screened.shape
    bands = pair_left.shape[1]
    nk = momentum_index.shape[0]
    s.entries = float(nk * bands)
    total = groups * s.rows
    state = ((s.rows, bands), F32)
    pairs = (s.rows * width // CORES // LANES + s.chains) // 2
    packet = ((groups * parts, pairs, 2, LANES), BF)

    def exchange(x, axes):
        return lax.all_to_all(x, axes, 0, 0, tiled=True)

    def across(x, axis, size, distance):
        return lax.ppermute(x, axis, [(i, i ^ distance) for i in range(size)])

    def swap(pieces, axis="kpt"):
        return [pieces[0]] + [
            across(piece, axis, len(pieces), at) for at, piece in enumerate(pieces) if at
        ]

    screened = pltpu.with_memory_space_constraint(screened, pltpu.VMEM)
    inputs = tuple(
        pltpu.with_memory_space_constraint(x, pltpu.HBM)
        for x in (current, previous, energies)
    )
    piece = ((2 * s.rows, 2 * band_block), F32)
    (start,) = call(
        functools.partial(begin_kernel, s),
        inputs,
        [piece],
        "begin",
        specs=[HBM] * len(inputs),
        scratch=[pltpu.VMEM(x.shape, x.dtype) for x in inputs]
        + [pltpu.SemaphoreType.DMA((len(inputs),))],
        cost=COVER,
    )
    (start,) = call(
        functools.partial(stack_kernel, s),
        (start, across(start, "core", CORES, 1)),
        [((CORES * 2 * s.rows, 2 * band_block), F32)],
        "stack",
    )
    (pick,) = call(
        functools.partial(pick_kernel, s),
        (momentum_index,),
        [((total, s.transfers * 3 * total), BF)],
        "pick",
    )
    start = swap([start] * s.chips, "z")
    sent, vector, earlier, levels = call(
        functools.partial(unpack_kernel, s),
        (*start, pair_right, pick),
        [packet, state, state, state],
        "unpack",
        cost=COVER,
    )
    scalars = []
    before = work = None
    for step in range(STEPS):
        first, keep = step == 0, step < STEPS - 1
        got = exchange(sent, ("kpt", "z", "core"))
        other = across(got, "core", CORES, 1)
        image = ((s.transfers, total, width), F32)
        (half,) = call(
            functools.partial(half_kernel, s), (got, screened), [image], "half", cost=COVER
        )
        args = (half, got, other) + (() if first else (before,)) + (screened, pick)
        outs = [((s.rows, width), F32)] * groups
        outs += [] if first else [((s.rows, LANES), F32)]
        outs += [image] if keep else []
        results = call(
            functools.partial(screen_kernel, s, first, keep),
            args,
            outs,
            "screen",
            scratch=[pltpu.VMEM((total, width), F32)],
        )
        if not first:
            scalars.append(results[groups])
        if keep:
            before = results[-1]
        (direct,) = call(
            functools.partial(field_kernel, s, first),
            (*swap(results[:groups])[::-1], pair_left),
            [state],
            "field",
        )
        (direct,) = call(
            functools.partial(pair_kernel, s),
            (direct, across(direct, "core", CORES, 1)),
            [((s.rows, bands), BF)],
            "pair",
        )
        direct = swap([direct] * s.chips, "z")
        if first:
            sent, work = call(
                functools.partial(first_kernel, s),
                (*direct, vector, earlier, levels, previous_beta[None], pair_right),
                [packet, state],
                "apply",
            )
        elif keep:
            sent, work, vector = call(
                functools.partial(later_kernel, s),
                (*direct, work, vector, levels, scalars[-1], pair_right),
                [packet, state, state],
                "apply",
            )
        else:
            sent, work, vector = call(
                functools.partial(last_kernel, s),
                (*direct, work, vector, levels, scalars[-1]),
                [((s.rows, LANES), F32), state, state],
                "apply",
            )
    sums = swap([sent] * groups)
    own = (current.shape, F32)
    terms = ((s.chains, STEPS), F32)
    block = ((s.rows, band_block), F32)
    own_work, own_vector, known, prior = call(
        functools.partial(own_kernel, s),
        (work, vector, *scalars),
        [block, block, ((s.rows, LANES), F32), own],
        "own",
        out_specs=[VMEM] * 3 + [HBM],
        scratch=[pltpu.VMEM(*own), pltpu.SemaphoreType.DMA((1,))],
    )
    last, alphas, betas = call(
        functools.partial(end_kernel, s),
        (*sums, own_work, own_vector, known),
        [own, terms, terms],
        "end",
        out_specs=[HBM] * 3,
        scratch=[pltpu.VMEM(*x) for x in (own, terms, terms)]
        + [pltpu.SemaphoreType.DMA((3,))],
    )
    return last, prior, alphas, betas


def solution(mesh):
    groups, parts = mesh.shape["kpt"], mesh.shape["pw"]
    devices = mesh.devices.reshape(groups, parts // CORES, CORES)
    pw = ("z", "core")
    return jax.shard_map(
        functools.partial(on_device, groups, parts),
        mesh=jax.sharding.Mesh(devices, ("kpt", *pw)),
        in_specs=(
            P("kpt", pw),
            P(None, "kpt", pw),
            P(None, "kpt", pw),
            P(),
            P("kpt", None, pw),
            P("kpt", None, pw),
            P("kpt", pw, None),
            P(),
        ),
        out_specs=(P(None, "kpt", pw), P(None, "kpt", pw), P(), P()),
        check_vma=False,
    )
```

```python
import functools

import jax
import jax.numpy as jnp
from jax import lax
from jax.experimental import pallas as pl
from jax.experimental.pallas import tpu as pltpu
from jax.sharding import PartitionSpec as P

STEPS = 3
EPSILON = 1e-06
COVER = 10_000_000_000
LANES = 128
CORES = 2
BF, F32 = jnp.bfloat16, jnp.float32


def iota(shape, axis):
    return lax.broadcasted_iota(jnp.int32, shape, axis)


def high_low(x):
    high = x.astype(BF)
    return high, (x - high.astype(F32)).astype(BF)


def three_pieces(x):
    high = x.astype(BF).astype(F32)
    rest = x - high
    middle = rest.astype(BF).astype(F32)
    return high, middle, (rest - middle).astype(BF).astype(F32)


def chain_rows(x, chains):
    rows = x.shape[0] // chains
    parts = []
    for n in range(chains):
        part = jnp.sum(x[n * rows : (n + 1) * rows], axis=(0, 1), keepdims=True)
        parts.append(jnp.broadcast_to(part, (rows, 1)))
    return jnp.concatenate(parts, axis=0)


def copy_all(sources, targets, sems):
    started = [
        pltpu.make_async_copy(source, target, sems.at[at])
        for at, (source, target) in enumerate(zip(sources, targets))
    ]
    for copy in started:
        copy.start()
    for copy in started:
        copy.wait()


def begin_kernel(s, *refs):
    sources, out_ref, held, sems = refs[:3], refs[3], refs[4:7], refs[7]
    copy_all(sources, held, sems)
    current_ref, previous_ref, energies_ref = held
    both = []
    for ref in (current_ref, previous_ref):
        both.append(jnp.concatenate([ref[n] for n in range(s.chains)], axis=0))
    levels = jnp.concatenate([energies_ref[...]] * s.chains, axis=0)
    out_ref[...] = jnp.concatenate(
        [jnp.concatenate(both, axis=1), jnp.concatenate([levels] * 2, axis=1)], axis=0
    )


def stack_kernel(s, own_ref, other_ref, out_ref):
    core = lax.axis_index("core")
    height = own_ref.shape[0]
    for c in range(CORES):
        value = jnp.where(core == c, own_ref[...], other_ref[...])
        out_ref[c * height : (c + 1) * height, :] = value


def pick_kernel(s, mi_ref, pick_ref):
    rows = s.rows
    mi = mi_ref[...].astype(F32).astype(BF)
    total, nk = s.groups * rows, mi.shape[0]

    def kpoint(r):
        return (r // rows) * s.kpoints + r % s.kpoints

    def chain(r):
        return (r % rows) // s.kpoints

    left = (kpoint(iota((total, nk), 0)) == iota((total, nk), 1)).astype(F32).astype(BF)
    right = (iota((nk, total), 0) == kpoint(iota((nk, total), 1))).astype(F32).astype(BF)
    spread = jnp.dot(left, mi, preferred_element_type=F32)
    spread = jnp.dot(spread.astype(BF), right, preferred_element_type=F32)
    same = chain(iota((total, total), 0)) == chain(iota((total, total), 1))
    for q in range(s.transfers):
        wanted = (lax.axis_index("kpt") * s.transfers + q).astype(F32)
        one = jnp.where(jnp.logical_and(spread == wanted, same), 1.0, 0.0).astype(BF)
        for piece in range(3):
            at = (q * 3 + piece) * total
            pick_ref[:, at : at + total] = one


def unpack_kernel(s, *refs):
    right_ref, _, packet_ref, vector_ref, earlier_ref, levels_ref = refs[s.chips :]
    rows = s.rows
    width = refs[0].shape[1] // 2
    pieces = in_order(lax.axis_index("z"), [ref[...] for ref in refs[: s.chips]])
    for ref, row, lane in ((vector_ref, 0, 0), (earlier_ref, 0, width), (levels_ref, rows, 0)):
        blocks = []
        for piece in pieces:
            for c in range(CORES):
                at = 2 * rows * c + row
                blocks.append(piece[at : at + rows, lane : lane + width])
        ref[...] = jnp.concatenate(blocks, axis=1)
    density = project(s, (vector_ref[...].astype(BF),), right_ref)
    send(s, density, jnp.zeros((rows, LANES), F32), packet_ref)


def project(s, parts, right_ref):
    x = jnp.concatenate([part.astype(F32) for part in parts], axis=0)
    total = None
    for k in range(s.kpoints):
        own = iota(x.shape, 0) % s.kpoints == k
        masked = jnp.where(own, x, 0.0).astype(BF)
        part = jnp.dot(masked, right_ref[k], preferred_element_type=F32)
        total = part if total is None else total + part
    return sum(total[at : at + s.rows] for at in range(0, x.shape[0], s.rows))


def send(s, density, sums, packet_ref):
    half = density.shape[1] // CORES
    k = s.kpoints
    ends = [sums[n * k : n * k + 1] for n in range(s.chains)]
    for c in range(CORES):
        blocks = [density[:, at : at + LANES] for at in range(c * half, (c + 1) * half, LANES)]
        value = jnp.concatenate(blocks + ends, axis=0).astype(BF)
        value = value.reshape(packet_ref.shape[1:])
        for d in range(c, packet_ref.shape[0], CORES):
            packet_ref[d] = value


def received(s, packet_ref, d):
    value = packet_ref[d].reshape(-1, LANES).astype(F32)
    height = value.shape[0] - s.chains
    blocks = [value[at : at + s.rows] for at in range(0, height, s.rows)]
    sums = [
        jnp.broadcast_to(value[height + n : height + n + 1], (s.kpoints, LANES))
        for n in range(s.chains)
    ]
    return jnp.concatenate(blocks, axis=1), jnp.concatenate(sums, axis=0)


def pair_kernel(s, own_ref, other_ref, out_ref):
    out_ref[...] = (own_ref[...] + other_ref[...]).astype(BF)


def apply_step(s, refs, vector, earlier, levels, beta):
    pieces = [ref[...].astype(F32) for ref in refs]
    direct = sum(in_order(lax.axis_index("z"), pieces))
    applied = levels * vector - direct - beta * earlier
    square = chain_rows(vector * vector, s.chains)
    cross = chain_rows(vector * applied, s.chains)
    shift = jnp.where(square > 0.0, cross / jnp.where(square > 0.0, square, 1.0), 0.0)
    shift = shift.astype(BF).astype(F32)
    work = applied - shift * vector
    sums = (
        square,
        chain_rows(work * vector, s.chains),
        chain_rows(work * work, s.chains),
        shift,
    )
    lane = iota((s.rows, LANES), 1)
    value = jnp.zeros((s.rows, LANES), F32)
    for at, item in enumerate(sums):
        value = jnp.where(lane % 4 == at, item, value)
    high, middle, low = three_pieces(value)
    packed = jnp.where(lane < 4, high, jnp.where(lane < 8, middle, low))
    return work, packed


def read_sums(s, tiles):
    square, cross, work, shift = [], [], [], []
    for tile in tiles:
        value = tile[:, 0:4] + tile[:, 4:8] + tile[:, 8:12]
        for at, into in enumerate((square, cross, work, shift)):
            into.append(value[:, at : at + 1])
    alpha = sum(c + h * q for c, h, q in zip(cross, shift, square)) / s.entries
    offsets = [h - alpha for h in shift]
    mean = sum(
        w + 2.0 * o * c + o * (o * q) for w, o, c, q in zip(work, offsets, cross, square)
    )
    beta = jnp.sqrt(jnp.maximum(mean / s.entries, 0.0) + EPSILON)
    return alpha, beta, offsets


def later_kernel(s, *refs):
    direct_refs, refs = refs[: s.chips], refs[s.chips :]
    work_ref, vector_ref, levels_ref, scalars_ref, right_ref = refs[:5]
    packet_ref, new_work_ref, new_vector_ref = refs[5:]
    vector, beta = advance(work_ref, vector_ref, scalars_ref)
    new_vector_ref[...] = vector
    work, packed = apply_step(s, direct_refs, vector, vector_ref[...], levels_ref[...], beta)
    new_work_ref[...] = work
    finish_packet(s, work, packed, right_ref, packet_ref)


def first_kernel(s, *refs):
    direct_refs, refs = refs[: s.chips], refs[s.chips :]
    vector_ref, earlier_ref, levels_ref, beta_ref, right_ref = refs[:5]
    packet_ref, new_work_ref = refs[5:]
    beta = first_beta(s, beta_ref)
    work, packed = apply_step(
        s, direct_refs, vector_ref[...], earlier_ref[...], levels_ref[...], beta
    )
    new_work_ref[...] = work
    finish_packet(s, work, packed, right_ref, packet_ref)


def first_beta(s, beta_ref):
    row = iota((s.rows, 1), 0) // s.kpoints
    beta = jnp.zeros((s.rows, 1), F32)
    for n in range(s.chains):
        beta = jnp.where(row == n, beta_ref[:, n : n + 1], beta)
    return beta


def advance(work_ref, vector_ref, scalars_ref):
    beta = scalars_ref[:, 1:2]
    offset = scalars_ref[:, 2:3]
    return (work_ref[...] + offset * vector_ref[...]) / beta, beta


def finish_packet(s, work, packed, right_ref, packet_ref):
    send(s, project(s, high_low(work), right_ref), packed, packet_ref)


def last_kernel(s, *refs):
    direct_refs, refs = refs[: s.chips], refs[s.chips :]
    work_ref, vector_ref, levels_ref, scalars_ref = refs[:4]
    packet_ref, new_work_ref, new_vector_ref = refs[4:]
    vector, beta = advance(work_ref, vector_ref, scalars_ref)
    new_vector_ref[...] = vector
    work, packed = apply_step(s, direct_refs, vector, vector_ref[...], levels_ref[...], beta)
    new_work_ref[...] = work
    packet_ref[...] = packed


def in_order(me, pieces):
    ordered = []
    for source in range(len(pieces)):
        piece = pieces[0]
        for distance in range(1, len(pieces)):
            piece = jnp.where((me ^ source) == distance, pieces[distance], piece)
        ordered.append(piece)
    return ordered


def own_kernel(s, work_ref, vector_ref, *refs):
    scalar_refs = refs[:-6]
    own_work_ref, own_vector_ref, terms_ref, prior_ref, prior, sem = refs[-6:]
    width = own_work_ref.shape[1]
    me = lax.axis_index("z") * CORES + lax.axis_index("core")
    for source, target in ((work_ref, own_work_ref), (vector_ref, own_vector_ref)):
        own = source[:, :width]
        for b in range(1, s.parts):
            own = jnp.where(me == b, source[:, b * width : (b + 1) * width], own)
        target[...] = own
    for n in range(s.chains):
        prior[n] = own_vector_ref[n * s.kpoints : (n + 1) * s.kpoints, :]
    copy = pltpu.make_async_copy(prior, prior_ref, sem.at[0])
    copy.start()
    lane = iota((s.rows, LANES), 1)
    terms = jnp.zeros((s.rows, LANES), F32)
    for at, ref in enumerate(scalar_refs):
        terms = jnp.where(lane == at, ref[:, 0:1], terms)
        terms = jnp.where(lane == STEPS + at, ref[:, 1:2], terms)
    terms_ref[...] = terms
    copy.wait()


def end_kernel(s, *refs):
    sums, refs = [ref[...] for ref in refs[: s.groups]], refs[s.groups :]
    work_ref, vector_ref, terms_ref = refs[:3]
    targets, held, sems = refs[3:6], refs[6:9], refs[9]
    last_ref, alphas_ref, betas_ref = held
    alpha, beta, offsets = read_sums(s, in_order(lax.axis_index("kpt"), sums))
    offset = own_offset(s, offsets)
    last = (work_ref[...] + offset * vector_ref[...]) / beta
    lane = iota((s.rows, LANES), 1)
    terms = jnp.where(lane == STEPS - 1, alpha, terms_ref[...])
    terms = jnp.where(lane == 2 * STEPS - 1, beta, terms)
    k = s.kpoints
    for n in range(s.chains):
        last_ref[n] = last[n * k : (n + 1) * k]
        alphas_ref[n : n + 1, :] = terms[n * k : n * k + 1, :STEPS]
        betas_ref[n : n + 1, :] = terms[n * k : n * k + 1, STEPS : 2 * STEPS]
    copy_all(held, targets, sems)


def own_offset(s, offsets):
    me = lax.axis_index("kpt")
    own = jnp.zeros_like(offsets[0])
    for a in range(s.groups):
        own = jnp.where(me == a, offsets[a], own)
    return own


def images(s, packet_ref, screened_ref, other):
    columns = []
    for b in range(s.parts):
        blocks = [received(s, packet_ref, a * s.parts + b)[0] for a in range(s.groups)]
        columns.append(jnp.concatenate(blocks, axis=0).astype(BF))
    half = columns[0].shape[1]
    core = lax.axis_index("core") ^ other
    result = []
    for q in range(s.transfers):
        image = None
        for b in range(s.parts):
            at = (b * CORES + core) * half
            piece = lax.dot_general(
                screened_ref[q, :, pl.ds(pl.multiple_of(at, half), half)],
                columns[b],
                (((1,), (1,)), ((), ())),
                preferred_element_type=F32,
            )
            image = piece if image is None else image + piece
        result.append(image.T)
    return result


def half_kernel(s, packet_ref, screened_ref, image_ref):
    for q, image in enumerate(images(s, packet_ref, screened_ref, 0)):
        image_ref[q] = image


def screen_kernel(s, first, keep, *refs):
    refs = list(refs)
    half_ref = refs.pop(0)
    packet_refs = refs[:CORES]
    del refs[:CORES]
    before_ref = None if first else refs.pop(0)
    screened_ref, pick_ref = refs[:2]
    out_refs = refs[2 : 2 + s.groups]
    del refs[: 2 + s.groups]
    scalars_ref = None if first else refs.pop(0)
    image_ref = refs.pop(0) if keep else None
    (field_ref,) = refs
    rows = s.rows
    if not first:
        tiles = [received(s, packet_refs[0], a * s.parts)[1] for a in range(s.groups)]
        alpha, beta, offsets = read_sums(s, tiles)
        scale = 1.0 / beta
        lane = iota((rows, LANES), 1)
        scalars_ref[...] = jnp.where(
            lane == 0, alpha, jnp.where(lane == 1, beta, own_offset(s, offsets))
        )
        shifts = jnp.concatenate(offsets, axis=0)
        scales = jnp.concatenate([scale] * s.groups, axis=0)
    pieces = []
    for q, image in enumerate(images(s, packet_refs[1], screened_ref, 1)):
        image = image + half_ref[q]
        if not first:
            image = (image + shifts * before_ref[q]) * scales
        if keep:
            image_ref[q] = image
        pieces.extend(three_pieces(image))
    stacked = jnp.concatenate([piece.astype(BF) for piece in pieces], axis=0)
    field_ref[...] = jnp.dot(pick_ref[...], stacked, preferred_element_type=F32)
    mine = lax.axis_index("kpt")
    for a in range(s.groups):
        out_refs[a][...] = field_ref[pl.ds(pl.multiple_of((mine ^ a) * rows, rows), rows), :]


def field_kernel(s, first, *refs):
    left_ref, out_ref = refs[-2:]
    field = refs[0][...]
    for ref in refs[1:-2]:
        field = field + ref[...]
    parts = (field.astype(BF),) if first else high_low(field)
    stacked = jnp.concatenate([p.astype(F32) for p in parts], axis=0).astype(BF)
    rows = s.rows
    direct = None
    for k in range(s.kpoints):
        image = lax.dot_general(
            stacked, left_ref[k], (((1,), (1,)), ((), ())), preferred_element_type=F32
        )
        if not first:
            image = image[:rows] + image[rows:]
        own = iota(image.shape, 0) % s.kpoints == k
        direct = jnp.where(own, image, 0.0 if direct is None else direct)
    out_ref[...] = direct


class Sizes:
    pass


VMEM = pl.BlockSpec(memory_space=pltpu.VMEM)
HBM = pl.BlockSpec(memory_space=pltpu.HBM)


def call(body, args, outs, name, specs=None, out_specs=None, scratch=(), limit=24, cost=0):
    return pl.pallas_call(
        body,
        out_shape=[jax.ShapeDtypeStruct(shape, dtype) for shape, dtype in outs],
        in_specs=specs or [VMEM] * len(args),
        out_specs=out_specs or [VMEM] * len(outs),
        scratch_shapes=list(scratch),
        compiler_params=pltpu.CompilerParams(vmem_limit_bytes=limit * 1024 * 1024),
        name=name,
        cost_estimate=pl.CostEstimate(
            flops=cost, bytes_accessed=cost // 256, transcendentals=0
        ),
    )(*args)


def on_device(
    groups, parts,
    energies, current, previous, previous_beta, pair_left, pair_right, screened, momentum_index
):
    s = Sizes()
    s.groups, s.parts, s.chips = groups, parts, parts // CORES
    s.chains, s.kpoints, band_block = current.shape
    s.rows = s.chains * s.kpoints
    s.transfers, width, waves = screened.shape
    bands = pair_left.shape[1]
    nk = momentum_index.shape[0]
    s.entries = float(nk * bands)
    total = groups * s.rows
    state = ((s.rows, bands), F32)
    pairs = (s.rows * width // CORES // LANES + s.chains) // 2
    packet = ((groups * parts, pairs, 2, LANES), BF)

    def exchange(x, axes):
        return lax.all_to_all(x, axes, 0, 0, tiled=True)

    def across(x, axis, size, distance):
        return lax.ppermute(x, axis, [(i, i ^ distance) for i in range(size)])

    def farthest_first(pieces):
        order = sorted(range(len(pieces)), key=lambda at: -at.bit_count())
        return [pieces[at] for at in order]

    def swap(pieces, axis="kpt"):
        return [pieces[0]] + [
            across(piece, axis, len(pieces), at) for at, piece in enumerate(pieces) if at
        ]

    screened = pltpu.with_memory_space_constraint(screened, pltpu.VMEM)
    inputs = tuple(
        pltpu.with_memory_space_constraint(x, pltpu.HBM)
        for x in (current, previous, energies)
    )
    piece = ((2 * s.rows, 2 * band_block), F32)
    (start,) = call(
        functools.partial(begin_kernel, s),
        inputs,
        [piece],
        "begin",
        specs=[HBM] * len(inputs),
        scratch=[pltpu.VMEM(x.shape, x.dtype) for x in inputs]
        + [pltpu.SemaphoreType.DMA((len(inputs),))],
        cost=COVER,
    )
    (start,) = call(
        functools.partial(stack_kernel, s),
        (start, across(start, "core", CORES, 1)),
        [((CORES * 2 * s.rows, 2 * band_block), F32)],
        "stack",
    )
    (pick,) = call(
        functools.partial(pick_kernel, s),
        (momentum_index,),
        [((total, s.transfers * 3 * total), BF)],
        "pick",
    )
    start = swap([start] * s.chips, "z")
    sent, vector, earlier, levels = call(
        functools.partial(unpack_kernel, s),
        (*start, pair_right, pick),
        [packet, state, state, state],
        "unpack",
        cost=COVER,
    )
    scalars = []
    before = work = None
    for step in range(STEPS):
        first, keep = step == 0, step < STEPS - 1
        got = exchange(sent, ("kpt", "z", "core"))
        other = across(got, "core", CORES, 1)
        image = ((s.transfers, total, width), F32)
        (half,) = call(
            functools.partial(half_kernel, s), (got, screened), [image], "half", cost=COVER
        )
        args = (half, got, other) + (() if first else (before,)) + (screened, pick)
        outs = [((s.rows, width), F32)] * groups
        outs += [] if first else [((s.rows, LANES), F32)]
        outs += [image] if keep else []
        results = call(
            functools.partial(screen_kernel, s, first, keep),
            args,
            outs,
            "screen",
            scratch=[pltpu.VMEM((total, width), F32)],
        )
        if not first:
            scalars.append(results[groups])
        if keep:
            before = results[-1]
        (direct,) = call(
            functools.partial(field_kernel, s, first),
            (*farthest_first(swap(results[:groups])), pair_left),
            [state],
            "field",
        )
        (direct,) = call(
            functools.partial(pair_kernel, s),
            (direct, across(direct, "core", CORES, 1)),
            [((s.rows, bands), BF)],
            "pair",
        )
        direct = swap([direct] * s.chips, "z")
        if first:
            sent, work = call(
                functools.partial(first_kernel, s),
                (*direct, vector, earlier, levels, previous_beta[None], pair_right),
                [packet, state],
                "apply",
            )
        elif keep:
            sent, work, vector = call(
                functools.partial(later_kernel, s),
                (*direct, work, vector, levels, scalars[-1], pair_right),
                [packet, state, state],
                "apply",
            )
        else:
            sent, work, vector = call(
                functools.partial(last_kernel, s),
                (*direct, work, vector, levels, scalars[-1]),
                [((s.rows, LANES), F32), state, state],
                "apply",
            )
    sums = swap([sent] * groups)
    own = (current.shape, F32)
    terms = ((s.chains, STEPS), F32)
    block = ((s.rows, band_block), F32)
    own_work, own_vector, known, prior = call(
        functools.partial(own_kernel, s),
        (work, vector, *scalars),
        [block, block, ((s.rows, LANES), F32), own],
        "own",
        out_specs=[VMEM] * 3 + [HBM],
        scratch=[pltpu.VMEM(*own), pltpu.SemaphoreType.DMA((1,))],
    )
    last, alphas, betas = call(
        functools.partial(end_kernel, s),
        (*sums, own_work, own_vector, known),
        [own, terms, terms],
        "end",
        out_specs=[HBM] * 3,
        scratch=[pltpu.VMEM(*x) for x in (own, terms, terms)]
        + [pltpu.SemaphoreType.DMA((3,))],
    )
    return last, prior, alphas, betas


def solution(mesh):
    groups, parts = mesh.shape["kpt"], mesh.shape["pw"]
    devices = mesh.devices.reshape(groups, parts // CORES, CORES)
    pw = ("z", "core")
    return jax.shard_map(
        functools.partial(on_device, groups, parts),
        mesh=jax.sharding.Mesh(devices, ("kpt", *pw)),
        in_specs=(
            P("kpt", pw),
            P(None, "kpt", pw),
            P(None, "kpt", pw),
            P(),
            P("kpt", None, pw),
            P("kpt", None, pw),
            P("kpt", pw, None),
            P(),
        ),
        out_specs=(P(None, "kpt", pw), P(None, "kpt", pw), P(), P()),
        check_vma=False,
    )
```

```python
import functools

import jax
import jax.numpy as jnp
from jax import lax
from jax.experimental import pallas as pl
from jax.experimental.pallas import tpu as pltpu
from jax.sharding import PartitionSpec as P

STEPS = 3
EPSILON = 1e-06
COVER = 10_000_000_000
LANES = 128
CORES = 2
BF, F32 = jnp.bfloat16, jnp.float32


def iota(shape, axis):
    return lax.broadcasted_iota(jnp.int32, shape, axis)


def high_low(x):
    high = x.astype(BF)
    return high, (x - high.astype(F32)).astype(BF)


def three_pieces(x):
    high = x.astype(BF).astype(F32)
    rest = x - high
    middle = rest.astype(BF).astype(F32)
    return high, middle, (rest - middle).astype(BF).astype(F32)


def chain_rows(x, chains):
    rows = x.shape[0] // chains
    parts = []
    for n in range(chains):
        part = jnp.sum(x[n * rows : (n + 1) * rows], axis=(0, 1), keepdims=True)
        parts.append(jnp.broadcast_to(part, (rows, 1)))
    return jnp.concatenate(parts, axis=0)


def copy_all(sources, targets, sems):
    started = [
        pltpu.make_async_copy(source, target, sems.at[at])
        for at, (source, target) in enumerate(zip(sources, targets))
    ]
    for copy in started:
        copy.start()
    for copy in started:
        copy.wait()


def begin_kernel(s, *refs):
    sources, out_ref, held, sems = refs[:3], refs[3], refs[4:7], refs[7]
    copy_all(sources, held, sems)
    current_ref, previous_ref, energies_ref = held
    both = []
    for ref in (current_ref, previous_ref):
        both.append(jnp.concatenate([ref[n] for n in range(s.chains)], axis=0))
    levels = jnp.concatenate([energies_ref[...]] * s.chains, axis=0)
    out_ref[...] = jnp.concatenate(
        [jnp.concatenate(both, axis=1), jnp.concatenate([levels] * 2, axis=1)], axis=0
    )


def stack_kernel(s, own_ref, other_ref, out_ref):
    core = lax.axis_index("core")
    height = own_ref.shape[0]
    for c in range(CORES):
        value = jnp.where(core == c, own_ref[...], other_ref[...])
        out_ref[c * height : (c + 1) * height, :] = value


def pick_kernel(s, mi_ref, pick_ref):
    rows = s.rows
    mi = mi_ref[...].astype(F32).astype(BF)
    total, nk = s.groups * rows, mi.shape[0]

    def kpoint(r):
        return (r // rows) * s.kpoints + r % s.kpoints

    def chain(r):
        return (r % rows) // s.kpoints

    left = (kpoint(iota((total, nk), 0)) == iota((total, nk), 1)).astype(F32).astype(BF)
    right = (iota((nk, total), 0) == kpoint(iota((nk, total), 1))).astype(F32).astype(BF)
    spread = jnp.dot(left, mi, preferred_element_type=F32)
    spread = jnp.dot(spread.astype(BF), right, preferred_element_type=F32)
    same = chain(iota((total, total), 0)) == chain(iota((total, total), 1))
    for q in range(s.transfers):
        wanted = (lax.axis_index("kpt") * s.transfers + q).astype(F32)
        one = jnp.where(jnp.logical_and(spread == wanted, same), 1.0, 0.0).astype(BF)
        for piece in range(3):
            at = (q * 3 + piece) * total
            pick_ref[:, at : at + total] = one


def unpack_kernel(s, *refs):
    right_ref, _, packet_ref, vector_ref, earlier_ref, levels_ref, density_ref = refs[s.chips :]
    rows = s.rows
    width = refs[0].shape[1] // 2
    pieces = in_order(lax.axis_index("z"), [ref[...] for ref in refs[: s.chips]])
    for ref, row, lane in ((vector_ref, 0, 0), (earlier_ref, 0, width), (levels_ref, rows, 0)):
        blocks = []
        for piece in pieces:
            for c in range(CORES):
                at = 2 * rows * c + row
                blocks.append(piece[at : at + rows, lane : lane + width])
        ref[...] = jnp.concatenate(blocks, axis=1)
    high, low = project(s, vector_ref[...], right_ref)
    density_ref[...] = high + low
    send(s, high, jnp.zeros((rows, LANES), F32), packet_ref)


def project(s, x, right_ref):
    x = jnp.concatenate([part.astype(F32) for part in high_low(x)], axis=0)
    total = None
    for k in range(s.kpoints):
        own = iota(x.shape, 0) % s.kpoints == k
        masked = jnp.where(own, x, 0.0).astype(BF)
        part = jnp.dot(masked, right_ref[k], preferred_element_type=F32)
        total = part if total is None else total + part
    return total[: s.rows], total[s.rows :]


def send(s, density, sums, packet_ref):
    half = density.shape[1] // CORES
    k = s.kpoints
    ends = [sums[n * k : n * k + 1] for n in range(s.chains)]
    for c in range(CORES):
        blocks = [density[:, at : at + LANES] for at in range(c * half, (c + 1) * half, LANES)]
        value = jnp.concatenate(blocks + ends, axis=0).astype(BF)
        value = value.reshape(packet_ref.shape[1:])
        for d in range(c, packet_ref.shape[0], CORES):
            packet_ref[d] = value


def received(s, packet_ref, d):
    value = packet_ref[d].reshape(-1, LANES).astype(F32)
    height = value.shape[0] - s.chains
    blocks = [value[at : at + s.rows] for at in range(0, height, s.rows)]
    sums = [
        jnp.broadcast_to(value[height + n : height + n + 1], (s.kpoints, LANES))
        for n in range(s.chains)
    ]
    return jnp.concatenate(blocks, axis=1), jnp.concatenate(sums, axis=0)


def pair_kernel(s, own_ref, other_ref, out_ref):
    out_ref[...] = (own_ref[...] + other_ref[...]).astype(BF)


def apply_step(s, refs, vector, earlier, levels, beta):
    pieces = [ref[...].astype(F32) for ref in refs]
    direct = sum(in_order(lax.axis_index("z"), pieces))
    applied = levels * vector - direct - beta * earlier
    square = chain_rows(vector * vector, s.chains)
    cross = chain_rows(vector * applied, s.chains)
    shift = jnp.where(square > 0.0, cross / jnp.where(square > 0.0, square, 1.0), 0.0)
    sums = (square, cross, chain_rows(applied * applied, s.chains), shift)
    lane = iota((s.rows, LANES), 1)
    value = jnp.zeros((s.rows, LANES), F32)
    for at, item in enumerate(sums):
        value = jnp.where(lane % 4 == at, item, value)
    high, middle, low = three_pieces(value)
    packed = jnp.where(lane < 4, high, jnp.where(lane < 8, middle, low))
    return applied, shift, packed


def read_sums(s, tiles):
    square, cross, whole, shift = [], [], [], []
    for tile in tiles:
        value = tile[:, 0:4] + tile[:, 4:8] + tile[:, 8:12]
        for at, into in enumerate((square, cross, whole, shift)):
            into.append(value[:, at : at + 1])
    alpha = sum(cross) / s.entries
    offsets = [h - alpha for h in shift]
    mean = sum(w + alpha * (alpha * q - 2.0 * c) for w, c, q in zip(whole, cross, square))
    beta = jnp.sqrt(jnp.maximum(mean / s.entries, 0.0) + EPSILON)
    return alpha, beta, offsets


def later_kernel(s, *refs):
    direct_refs, refs = refs[: s.chips], refs[s.chips :]
    work_ref, vector_ref, levels_ref, scalars_ref = refs[:4]
    part_ref, density_ref, right_ref = refs[4:7]
    packet_ref, new_work_ref, new_vector_ref = refs[7:10]
    vector, beta = advance(work_ref, vector_ref, scalars_ref)
    density, _ = advance(part_ref, density_ref, scalars_ref)
    new_vector_ref[...] = vector
    step = apply_step(s, direct_refs, vector, vector_ref[...], levels_ref[...], beta)
    part = finish(s, step, vector, density, right_ref, packet_ref, new_work_ref)
    for ref, value in zip(refs[10:], (part, density)):
        ref[...] = value


def first_kernel(s, *refs):
    direct_refs, refs = refs[: s.chips], refs[s.chips :]
    vector_ref, earlier_ref, levels_ref, beta_ref, density_ref, right_ref = refs[:6]
    packet_ref, new_work_ref, new_part_ref = refs[6:]
    vector, beta = vector_ref[...], first_beta(s, beta_ref)
    step = apply_step(s, direct_refs, vector, earlier_ref[...], levels_ref[...], beta)
    density = density_ref[...]
    new_part_ref[...] = finish(s, step, vector, density, right_ref, packet_ref, new_work_ref)


def finish(s, step, vector, density, right_ref, packet_ref, new_work_ref):
    applied, shift, packed = step
    new_work_ref[...] = applied - shift * vector
    high, low = project(s, applied, right_ref)
    part = high + low - shift * density
    send(s, part, packed, packet_ref)
    return part


def first_beta(s, beta_ref):
    row = iota((s.rows, 1), 0) // s.kpoints
    beta = jnp.zeros((s.rows, 1), F32)
    for n in range(s.chains):
        beta = jnp.where(row == n, beta_ref[:, n : n + 1], beta)
    return beta


def advance(work_ref, vector_ref, scalars_ref):
    beta = scalars_ref[:, 1:2]
    offset = scalars_ref[:, 2:3]
    return (work_ref[...] + offset * vector_ref[...]) / beta, beta


def last_kernel(s, *refs):
    direct_refs, refs = refs[: s.chips], refs[s.chips :]
    work_ref, vector_ref, levels_ref, scalars_ref = refs[:4]
    packet_ref, new_work_ref, new_vector_ref = refs[4:]
    vector, beta = advance(work_ref, vector_ref, scalars_ref)
    new_vector_ref[...] = vector
    applied, shift, packed = apply_step(
        s, direct_refs, vector, vector_ref[...], levels_ref[...], beta
    )
    new_work_ref[...] = applied - shift * vector
    packet_ref[...] = packed


def in_order(me, pieces):
    ordered = []
    for source in range(len(pieces)):
        piece = pieces[0]
        for distance in range(1, len(pieces)):
            piece = jnp.where((me ^ source) == distance, pieces[distance], piece)
        ordered.append(piece)
    return ordered


def own_kernel(s, work_ref, vector_ref, *refs):
    scalar_refs = refs[:-6]
    own_work_ref, own_vector_ref, terms_ref, prior_ref, prior, sem = refs[-6:]
    width = own_work_ref.shape[1]
    me = lax.axis_index("z") * CORES + lax.axis_index("core")
    for source, target in ((work_ref, own_work_ref), (vector_ref, own_vector_ref)):
        own = source[:, :width]
        for b in range(1, s.parts):
            own = jnp.where(me == b, source[:, b * width : (b + 1) * width], own)
        target[...] = own
    for n in range(s.chains):
        prior[n] = own_vector_ref[n * s.kpoints : (n + 1) * s.kpoints, :]
    copy = pltpu.make_async_copy(prior, prior_ref, sem.at[0])
    copy.start()
    lane = iota((s.rows, LANES), 1)
    terms = jnp.zeros((s.rows, LANES), F32)
    for at, ref in enumerate(scalar_refs):
        terms = jnp.where(lane == at, ref[:, 0:1], terms)
        terms = jnp.where(lane == STEPS + at, ref[:, 1:2], terms)
    terms_ref[...] = terms
    copy.wait()


def end_kernel(s, *refs):
    sums, refs = [ref[...] for ref in refs[: s.groups]], refs[s.groups :]
    work_ref, vector_ref, terms_ref = refs[:3]
    targets, held, sems = refs[3:6], refs[6:9], refs[9]
    last_ref, alphas_ref, betas_ref = held
    alpha, beta, offsets = read_sums(s, in_order(lax.axis_index("kpt"), sums))
    offset = own_offset(s, offsets)
    last = (work_ref[...] + offset * vector_ref[...]) / beta
    lane = iota((s.rows, LANES), 1)
    terms = jnp.where(lane == STEPS - 1, alpha, terms_ref[...])
    terms = jnp.where(lane == 2 * STEPS - 1, beta, terms)
    k = s.kpoints
    for n in range(s.chains):
        last_ref[n] = last[n * k : (n + 1) * k]
        alphas_ref[n : n + 1, :] = terms[n * k : n * k + 1, :STEPS]
        betas_ref[n : n + 1, :] = terms[n * k : n * k + 1, STEPS : 2 * STEPS]
    copy_all(held, targets, sems)


def own_offset(s, offsets):
    me = lax.axis_index("kpt")
    own = jnp.zeros_like(offsets[0])
    for a in range(s.groups):
        own = jnp.where(me == a, offsets[a], own)
    return own


def images(s, packet_ref, screened_ref, other):
    columns = []
    for b in range(s.parts):
        blocks = [received(s, packet_ref, a * s.parts + b)[0] for a in range(s.groups)]
        columns.append(jnp.concatenate(blocks, axis=0).astype(BF))
    half = columns[0].shape[1]
    core = lax.axis_index("core") ^ other
    result = []
    for q in range(s.transfers):
        image = None
        for b in range(s.parts):
            at = (b * CORES + core) * half
            piece = lax.dot_general(
                screened_ref[q, :, pl.ds(pl.multiple_of(at, half), half)],
                columns[b],
                (((1,), (1,)), ((), ())),
                preferred_element_type=F32,
            )
            image = piece if image is None else image + piece
        result.append(image.T)
    return result


def half_kernel(s, packet_ref, screened_ref, image_ref):
    for q, image in enumerate(images(s, packet_ref, screened_ref, 0)):
        image_ref[q] = image


def screen_kernel(s, first, keep, *refs):
    refs = list(refs)
    half_ref = refs.pop(0)
    packet_refs = refs[:CORES]
    del refs[:CORES]
    before_ref = None if first else refs.pop(0)
    screened_ref, pick_ref = refs[:2]
    out_refs = refs[2 : 2 + s.groups]
    del refs[: 2 + s.groups]
    scalars_ref = None if first else refs.pop(0)
    image_ref = refs.pop(0) if keep else None
    (field_ref,) = refs
    rows = s.rows
    if not first:
        tiles = [received(s, packet_refs[0], a * s.parts)[1] for a in range(s.groups)]
        alpha, beta, offsets = read_sums(s, tiles)
        scale = 1.0 / beta
        lane = iota((rows, LANES), 1)
        scalars_ref[...] = jnp.where(
            lane == 0, alpha, jnp.where(lane == 1, beta, own_offset(s, offsets))
        )
        shifts = jnp.concatenate(offsets, axis=0)
        scales = jnp.concatenate([scale] * s.groups, axis=0)
    pieces = []
    for q, image in enumerate(images(s, packet_refs[1], screened_ref, 1)):
        image = image + half_ref[q]
        if not first:
            image = (image + shifts * before_ref[q]) * scales
        if keep:
            image_ref[q] = image
        pieces.extend(three_pieces(image))
    stacked = jnp.concatenate([piece.astype(BF) for piece in pieces], axis=0)
    field_ref[...] = jnp.dot(pick_ref[...], stacked, preferred_element_type=F32)
    mine = lax.axis_index("kpt")
    for a in range(s.groups):
        out_refs[a][...] = field_ref[pl.ds(pl.multiple_of((mine ^ a) * rows, rows), rows), :]


def field_kernel(s, first, *refs):
    left_ref, out_ref = refs[-2:]
    field = refs[0][...]
    for ref in refs[1:-2]:
        field = field + ref[...]
    parts = (field.astype(BF),) if first else high_low(field)
    stacked = jnp.concatenate([p.astype(F32) for p in parts], axis=0).astype(BF)
    rows = s.rows
    direct = None
    for k in range(s.kpoints):
        image = lax.dot_general(
            stacked, left_ref[k], (((1,), (1,)), ((), ())), preferred_element_type=F32
        )
        if not first:
            image = image[:rows] + image[rows:]
        own = iota(image.shape, 0) % s.kpoints == k
        direct = jnp.where(own, image, 0.0 if direct is None else direct)
    out_ref[...] = direct


class Sizes:
    pass


VMEM = pl.BlockSpec(memory_space=pltpu.VMEM)
HBM = pl.BlockSpec(memory_space=pltpu.HBM)


def call(body, args, outs, name, specs=None, out_specs=None, scratch=(), limit=24, cost=0):
    return pl.pallas_call(
        body,
        out_shape=[jax.ShapeDtypeStruct(shape, dtype) for shape, dtype in outs],
        in_specs=specs or [VMEM] * len(args),
        out_specs=out_specs or [VMEM] * len(outs),
        scratch_shapes=list(scratch),
        compiler_params=pltpu.CompilerParams(vmem_limit_bytes=limit * 1024 * 1024),
        name=name,
        cost_estimate=pl.CostEstimate(
            flops=cost, bytes_accessed=cost // 256, transcendentals=0
        ),
    )(*args)


def on_device(
    groups, parts,
    energies, current, previous, previous_beta, pair_left, pair_right, screened, momentum_index
):
    s = Sizes()
    s.groups, s.parts, s.chips = groups, parts, parts // CORES
    s.chains, s.kpoints, band_block = current.shape
    s.rows = s.chains * s.kpoints
    s.transfers, width, waves = screened.shape
    bands = pair_left.shape[1]
    nk = momentum_index.shape[0]
    s.entries = float(nk * bands)
    total = groups * s.rows
    state = ((s.rows, bands), F32)
    block = ((s.rows, width), F32)
    pairs = (s.rows * width // CORES // LANES + s.chains) // 2
    packet = ((groups * parts, pairs, 2, LANES), BF)

    def exchange(x, axes):
        return lax.all_to_all(x, axes, 0, 0, tiled=True)

    def across(x, axis, size, distance):
        return lax.ppermute(x, axis, [(i, i ^ distance) for i in range(size)])

    def farthest_first(pieces):
        order = sorted(range(len(pieces)), key=lambda at: -at.bit_count())
        return [pieces[at] for at in order]

    def swap(pieces, axis="kpt"):
        return [pieces[0]] + [
            across(piece, axis, len(pieces), at) for at, piece in enumerate(pieces) if at
        ]

    screened = pltpu.with_memory_space_constraint(screened, pltpu.VMEM)
    inputs = tuple(
        pltpu.with_memory_space_constraint(x, pltpu.HBM)
        for x in (current, previous, energies)
    )
    piece = ((2 * s.rows, 2 * band_block), F32)
    (start,) = call(
        functools.partial(begin_kernel, s),
        inputs,
        [piece],
        "begin",
        specs=[HBM] * len(inputs),
        scratch=[pltpu.VMEM(x.shape, x.dtype) for x in inputs]
        + [pltpu.SemaphoreType.DMA((len(inputs),))],
        cost=COVER,
    )
    (start,) = call(
        functools.partial(stack_kernel, s),
        (start, across(start, "core", CORES, 1)),
        [((CORES * 2 * s.rows, 2 * band_block), F32)],
        "stack",
    )
    (pick,) = call(
        functools.partial(pick_kernel, s),
        (momentum_index,),
        [((total, s.transfers * 3 * total), BF)],
        "pick",
    )
    start = swap([start] * s.chips, "z")
    sent, vector, earlier, levels, density = call(
        functools.partial(unpack_kernel, s),
        (*start, pair_right, pick),
        [packet, state, state, state, block],
        "unpack",
        cost=COVER,
    )
    scalars = []
    before = work = None
    for step in range(STEPS):
        first, keep = step == 0, step < STEPS - 1
        got = exchange(sent, ("kpt", "z", "core"))
        other = across(got, "core", CORES, 1)
        image = ((s.transfers, total, width), F32)
        (half,) = call(
            functools.partial(half_kernel, s), (got, screened), [image], "half", cost=COVER
        )
        args = (half, got, other) + (() if first else (before,)) + (screened, pick)
        outs = [((s.rows, width), F32)] * groups
        outs += [] if first else [((s.rows, LANES), F32)]
        outs += [image] if keep else []
        results = call(
            functools.partial(screen_kernel, s, first, keep),
            args,
            outs,
            "screen",
            scratch=[pltpu.VMEM((total, width), F32)],
        )
        if not first:
            scalars.append(results[groups])
        if keep:
            before = results[-1]
        (direct,) = call(
            functools.partial(field_kernel, s, first),
            (*farthest_first(swap(results[:groups])), pair_left),
            [state],
            "field",
        )
        (direct,) = call(
            functools.partial(pair_kernel, s),
            (direct, across(direct, "core", CORES, 1)),
            [((s.rows, bands), BF)],
            "pair",
        )
        direct = swap([direct] * s.chips, "z")
        if first:
            sent, work, part = call(
                functools.partial(first_kernel, s),
                (*direct, vector, earlier, levels, previous_beta[None], density, pair_right),
                [packet, state, block],
                "apply",
            )
        elif keep:
            sent, work, vector, *densities = call(
                functools.partial(later_kernel, s),
                (*direct, work, vector, levels, scalars[-1], part, density, pair_right),
                [packet, state, state] + [block, block] * (step < STEPS - 2),
                "apply",
            )
            part, density = densities or (None, None)
        else:
            sent, work, vector = call(
                functools.partial(last_kernel, s),
                (*direct, work, vector, levels, scalars[-1]),
                [((s.rows, LANES), F32), state, state],
                "apply",
            )
    sums = swap([sent] * groups)
    own = (current.shape, F32)
    terms = ((s.chains, STEPS), F32)
    bands_block = ((s.rows, band_block), F32)
    own_work, own_vector, known, prior = call(
        functools.partial(own_kernel, s),
        (work, vector, *scalars),
        [bands_block, bands_block, ((s.rows, LANES), F32), own],
        "own",
        out_specs=[VMEM] * 3 + [HBM],
        scratch=[pltpu.VMEM(*own), pltpu.SemaphoreType.DMA((1,))],
    )
    last, alphas, betas = call(
        functools.partial(end_kernel, s),
        (*sums, own_work, own_vector, known),
        [own, terms, terms],
        "end",
        out_specs=[HBM] * 3,
        scratch=[pltpu.VMEM(*x) for x in (own, terms, terms)]
        + [pltpu.SemaphoreType.DMA((3,))],
    )
    return last, prior, alphas, betas


def solution(mesh):
    groups, parts = mesh.shape["kpt"], mesh.shape["pw"]
    devices = mesh.devices.reshape(groups, parts // CORES, CORES)
    pw = ("z", "core")
    return jax.shard_map(
        functools.partial(on_device, groups, parts),
        mesh=jax.sharding.Mesh(devices, ("kpt", *pw)),
        in_specs=(
            P("kpt", pw),
            P(None, "kpt", pw),
            P(None, "kpt", pw),
            P(),
            P("kpt", None, pw),
            P("kpt", None, pw),
            P("kpt", pw, None),
            P(),
        ),
        out_specs=(P(None, "kpt", pw), P(None, "kpt", pw), P(), P()),
        check_vma=False,
    )
```

```python
import functools

import jax
import jax.numpy as jnp
from jax import lax
from jax.experimental import pallas as pl
from jax.experimental.pallas import tpu as pltpu
from jax.sharding import PartitionSpec as P

STEPS = 3
EPSILON = 1e-06
COVER = 10_000_000_000
LANES = 128
CORES = 2
BF, F32 = jnp.bfloat16, jnp.float32


def iota(shape, axis):
    return lax.broadcasted_iota(jnp.int32, shape, axis)


def high_low(x):
    high = x.astype(BF)
    return high, (x - high.astype(F32)).astype(BF)


def three_pieces(x):
    high = x.astype(BF).astype(F32)
    rest = x - high
    middle = rest.astype(BF).astype(F32)
    return high, middle, (rest - middle).astype(BF).astype(F32)


def chain_rows(x, chains):
    rows = x.shape[0] // chains
    parts = []
    for n in range(chains):
        part = jnp.sum(x[n * rows : (n + 1) * rows], axis=(0, 1), keepdims=True)
        parts.append(jnp.broadcast_to(part, (rows, 1)))
    return jnp.concatenate(parts, axis=0)


def copy_all(sources, targets, sems):
    started = [
        pltpu.make_async_copy(source, target, sems.at[at])
        for at, (source, target) in enumerate(zip(sources, targets))
    ]
    for copy in started:
        copy.start()
    for copy in started:
        copy.wait()


def begin_kernel(s, *refs):
    sources, out_ref, held, sems = refs[:3], refs[3], refs[4:7], refs[7]
    copy_all(sources, held, sems)
    current_ref, previous_ref, energies_ref = held
    both = []
    for ref in (current_ref, previous_ref):
        both.append(jnp.concatenate([ref[n] for n in range(s.chains)], axis=0))
    levels = jnp.concatenate([energies_ref[...]] * s.chains, axis=0)
    out_ref[...] = jnp.concatenate(
        [jnp.concatenate(both, axis=1), jnp.concatenate([levels] * 2, axis=1)], axis=0
    )


def stack_kernel(s, own_ref, other_ref, out_ref):
    core = lax.axis_index("core")
    half = own_ref.shape[1] // 2
    levels = []
    for c in range(CORES):
        value = jnp.where(core == c, own_ref[...], other_ref[...])
        out_ref[c * s.rows : (c + 1) * s.rows, :] = value[: s.rows]
        levels.append(value[s.rows :, :half])
    out_ref[CORES * s.rows :, :] = jnp.concatenate(levels, axis=1)


def pick_kernel(s, mi_ref, pick_ref):
    rows = s.rows
    mi = mi_ref[...].astype(F32).astype(BF)
    total, nk = s.groups * rows, mi.shape[0]

    def kpoint(r):
        return (r // rows) * s.kpoints + r % s.kpoints

    def chain(r):
        return (r % rows) // s.kpoints

    left = (kpoint(iota((total, nk), 0)) == iota((total, nk), 1)).astype(F32).astype(BF)
    right = (iota((nk, total), 0) == kpoint(iota((nk, total), 1))).astype(F32).astype(BF)
    spread = jnp.dot(left, mi, preferred_element_type=F32)
    spread = jnp.dot(spread.astype(BF), right, preferred_element_type=F32)
    same = chain(iota((total, total), 0)) == chain(iota((total, total), 1))
    for q in range(s.transfers):
        wanted = (lax.axis_index("kpt") * s.transfers + q).astype(F32)
        one = jnp.where(jnp.logical_and(spread == wanted, same), 1.0, 0.0).astype(BF)
        for piece in range(3):
            at = (q * 3 + piece) * total
            pick_ref[:, at : at + total] = one


def unpack_kernel(s, *refs):
    right_ref, _, packet_ref, vector_ref, earlier_ref, levels_ref, density_ref = refs[s.chips :]
    rows = s.rows
    width = refs[0].shape[1] // 2
    pieces = in_order(lax.axis_index("z"), [ref[...] for ref in refs[: s.chips]])
    for ref, lane in ((vector_ref, 0), (earlier_ref, width)):
        blocks = []
        for piece in pieces:
            for c in range(CORES):
                blocks.append(piece[rows * c : rows * (c + 1), lane : lane + width])
        ref[...] = jnp.concatenate(blocks, axis=1)
    levels_ref[...] = jnp.concatenate([piece[CORES * rows :] for piece in pieces], axis=1)
    high, low = project(s, vector_ref[...], right_ref)
    density_ref[...] = high + low
    send(s, high, jnp.zeros((rows, LANES), F32), packet_ref)


def project(s, x, right_ref):
    x = jnp.concatenate([part.astype(F32) for part in high_low(x)], axis=0)
    total = None
    for k in range(s.kpoints):
        own = iota(x.shape, 0) % s.kpoints == k
        masked = jnp.where(own, x, 0.0).astype(BF)
        part = jnp.dot(masked, right_ref[k], preferred_element_type=F32)
        total = part if total is None else total + part
    return total[: s.rows], total[s.rows :]


def send(s, density, sums, packet_ref):
    half = density.shape[1] // CORES
    k = s.kpoints
    ends = [sums[n * k : n * k + 1] for n in range(s.chains)]
    for c in range(CORES):
        blocks = [density[:, at : at + LANES] for at in range(c * half, (c + 1) * half, LANES)]
        value = jnp.concatenate(blocks + ends, axis=0).astype(BF)
        value = value.reshape(packet_ref.shape[1:])
        for d in range(c, packet_ref.shape[0], CORES):
            packet_ref[d] = value


def received(s, packet_ref, d):
    value = packet_ref[d].reshape(-1, LANES).astype(F32)
    height = value.shape[0] - s.chains
    blocks = [value[at : at + s.rows] for at in range(0, height, s.rows)]
    sums = [
        jnp.broadcast_to(value[height + n : height + n + 1], (s.kpoints, LANES))
        for n in range(s.chains)
    ]
    return jnp.concatenate(blocks, axis=1), jnp.concatenate(sums, axis=0)


def pair_kernel(s, own_ref, other_ref, out_ref):
    out_ref[...] = (own_ref[...] + other_ref[...]).astype(BF)


def apply_step(s, refs, vector, earlier, levels, beta):
    pieces = [ref[...].astype(F32) for ref in refs]
    direct = sum(in_order(lax.axis_index("z"), pieces))
    applied = levels * vector - direct - beta * earlier
    square = chain_rows(vector * vector, s.chains)
    cross = chain_rows(vector * applied, s.chains)
    shift = jnp.where(square > 0.0, cross / jnp.where(square > 0.0, square, 1.0), 0.0)
    sums = (square, cross, chain_rows(applied * applied, s.chains), shift)
    lane = iota((s.rows, LANES), 1)
    value = jnp.zeros((s.rows, LANES), F32)
    for at, item in enumerate(sums):
        value = jnp.where(lane % 4 == at, item, value)
    high, middle, low = three_pieces(value)
    packed = jnp.where(lane < 4, high, jnp.where(lane < 8, middle, low))
    return applied, shift, packed


def read_sums(s, tiles):
    square, cross, whole, shift = [], [], [], []
    for tile in tiles:
        value = tile[:, 0:4] + tile[:, 4:8] + tile[:, 8:12]
        for at, into in enumerate((square, cross, whole, shift)):
            into.append(value[:, at : at + 1])
    alpha = sum(cross) / s.entries
    offsets = [h - alpha for h in shift]
    mean = sum(w + alpha * (alpha * q - 2.0 * c) for w, c, q in zip(whole, cross, square))
    beta = jnp.sqrt(jnp.maximum(mean / s.entries, 0.0) + EPSILON)
    return alpha, beta, offsets


def later_kernel(s, *refs):
    direct_refs, refs = refs[: s.chips], refs[s.chips :]
    work_ref, vector_ref, levels_ref, scalars_ref = refs[:4]
    part_ref, density_ref, right_ref = refs[4:7]
    packet_ref, new_work_ref, new_vector_ref = refs[7:10]
    vector, beta = advance(work_ref, vector_ref, scalars_ref)
    density, _ = advance(part_ref, density_ref, scalars_ref)
    new_vector_ref[...] = vector
    step = apply_step(s, direct_refs, vector, vector_ref[...], levels_ref[...], beta)
    part = finish(s, step, vector, density, right_ref, packet_ref, new_work_ref)
    for ref, value in zip(refs[10:], (part, density)):
        ref[...] = value


def first_kernel(s, *refs):
    direct_refs, refs = refs[: s.chips], refs[s.chips :]
    vector_ref, earlier_ref, levels_ref, beta_ref, density_ref, right_ref = refs[:6]
    packet_ref, new_work_ref, new_part_ref = refs[6:]
    vector, beta = vector_ref[...], first_beta(s, beta_ref)
    step = apply_step(s, direct_refs, vector, earlier_ref[...], levels_ref[...], beta)
    density = density_ref[...]
    new_part_ref[...] = finish(s, step, vector, density, right_ref, packet_ref, new_work_ref)


def finish(s, step, vector, density, right_ref, packet_ref, new_work_ref):
    applied, shift, packed = step
    new_work_ref[...] = applied - shift * vector
    high, low = project(s, applied, right_ref)
    part = high + low - shift * density
    send(s, part, packed, packet_ref)
    return part


def first_beta(s, beta_ref):
    row = iota((s.rows, 1), 0) // s.kpoints
    beta = jnp.zeros((s.rows, 1), F32)
    for n in range(s.chains):
        beta = jnp.where(row == n, beta_ref[:, n : n + 1], beta)
    return beta


def advance(work_ref, vector_ref, scalars_ref):
    beta = scalars_ref[:, 1:2]
    offset = scalars_ref[:, 2:3]
    return (work_ref[...] + offset * vector_ref[...]) / beta, beta


def last_kernel(s, *refs):
    direct_refs, refs = refs[: s.chips], refs[s.chips :]
    work_ref, vector_ref, levels_ref, scalars_ref = refs[:4]
    packet_ref, new_work_ref, new_vector_ref = refs[4:]
    vector, beta = advance(work_ref, vector_ref, scalars_ref)
    new_vector_ref[...] = vector
    applied, shift, packed = apply_step(
        s, direct_refs, vector, vector_ref[...], levels_ref[...], beta
    )
    new_work_ref[...] = applied - shift * vector
    packet_ref[...] = packed


def in_order(me, pieces):
    ordered = []
    for source in range(len(pieces)):
        piece = pieces[0]
        for distance in range(1, len(pieces)):
            piece = jnp.where((me ^ source) == distance, pieces[distance], piece)
        ordered.append(piece)
    return ordered


def own_kernel(s, work_ref, vector_ref, *refs):
    scalar_refs = refs[:-6]
    own_work_ref, own_vector_ref, terms_ref, prior_ref, prior, sem = refs[-6:]
    width = own_work_ref.shape[1]
    me = lax.axis_index("z") * CORES + lax.axis_index("core")
    for source, target in ((work_ref, own_work_ref), (vector_ref, own_vector_ref)):
        own = source[:, :width]
        for b in range(1, s.parts):
            own = jnp.where(me == b, source[:, b * width : (b + 1) * width], own)
        target[...] = own
    for n in range(s.chains):
        prior[n] = own_vector_ref[n * s.kpoints : (n + 1) * s.kpoints, :]
    copy = pltpu.make_async_copy(prior, prior_ref, sem.at[0])
    copy.start()
    lane = iota((s.rows, LANES), 1)
    terms = jnp.zeros((s.rows, LANES), F32)
    for at, ref in enumerate(scalar_refs):
        terms = jnp.where(lane == at, ref[:, 0:1], terms)
        terms = jnp.where(lane == STEPS + at, ref[:, 1:2], terms)
    terms_ref[...] = terms
    copy.wait()


def end_kernel(s, *refs):
    sums, refs = [ref[...] for ref in refs[: s.groups]], refs[s.groups :]
    work_ref, vector_ref, terms_ref = refs[:3]
    targets, held, sems = refs[3:6], refs[6:9], refs[9]
    last_ref, alphas_ref, betas_ref = held
    alpha, beta, offsets = read_sums(s, in_order(lax.axis_index("kpt"), sums))
    offset = own_offset(s, offsets)
    last = (work_ref[...] + offset * vector_ref[...]) / beta
    lane = iota((s.rows, LANES), 1)
    terms = jnp.where(lane == STEPS - 1, alpha, terms_ref[...])
    terms = jnp.where(lane == 2 * STEPS - 1, beta, terms)
    k = s.kpoints
    for n in range(s.chains):
        last_ref[n] = last[n * k : (n + 1) * k]
        alphas_ref[n : n + 1, :] = terms[n * k : n * k + 1, :STEPS]
        betas_ref[n : n + 1, :] = terms[n * k : n * k + 1, STEPS : 2 * STEPS]
    copy_all(held, targets, sems)


def own_offset(s, offsets):
    me = lax.axis_index("kpt")
    own = jnp.zeros_like(offsets[0])
    for a in range(s.groups):
        own = jnp.where(me == a, offsets[a], own)
    return own


def images(s, packet_ref, screened_ref, other):
    columns = []
    for b in range(s.parts):
        blocks = [received(s, packet_ref, a * s.parts + b)[0] for a in range(s.groups)]
        columns.append(jnp.concatenate(blocks, axis=0).astype(BF))
    half = columns[0].shape[1]
    core = lax.axis_index("core") ^ other
    result = []
    for q in range(s.transfers):
        image = None
        for b in range(s.parts):
            at = (b * CORES + core) * half
            piece = lax.dot_general(
                screened_ref[q, :, pl.ds(pl.multiple_of(at, half), half)],
                columns[b],
                (((1,), (1,)), ((), ())),
                preferred_element_type=F32,
            )
            image = piece if image is None else image + piece
        result.append(image.T)
    return result


def half_kernel(s, packet_ref, screened_ref, image_ref):
    for q, image in enumerate(images(s, packet_ref, screened_ref, 0)):
        image_ref[q] = image


def screen_kernel(s, first, keep, *refs):
    refs = list(refs)
    half_ref = refs.pop(0)
    packet_refs = refs[:CORES]
    del refs[:CORES]
    before_ref = None if first else refs.pop(0)
    screened_ref, pick_ref = refs[:2]
    out_refs = refs[2 : 2 + s.groups]
    del refs[: 2 + s.groups]
    scalars_ref = None if first else refs.pop(0)
    image_ref = refs.pop(0) if keep else None
    (field_ref,) = refs
    rows = s.rows
    if not first:
        tiles = [received(s, packet_refs[0], a * s.parts)[1] for a in range(s.groups)]
        alpha, beta, offsets = read_sums(s, tiles)
        scale = 1.0 / beta
        lane = iota((rows, LANES), 1)
        scalars_ref[...] = jnp.where(
            lane == 0, alpha, jnp.where(lane == 1, beta, own_offset(s, offsets))
        )
        shifts = jnp.concatenate(offsets, axis=0)
        scales = jnp.concatenate([scale] * s.groups, axis=0)
    pieces = []
    for q, image in enumerate(images(s, packet_refs[1], screened_ref, 1)):
        image = image + half_ref[q]
        if not first:
            image = (image + shifts * before_ref[q]) * scales
        if keep:
            image_ref[q] = image
        pieces.extend(three_pieces(image))
    stacked = jnp.concatenate([piece.astype(BF) for piece in pieces], axis=0)
    field_ref[...] = jnp.dot(pick_ref[...], stacked, preferred_element_type=F32)
    mine = lax.axis_index("kpt")
    for a in range(s.groups):
        at = pl.ds(pl.multiple_of((mine ^ a) * rows, rows), rows)
        out_refs[a][...] = field_ref[at, :].astype(out_refs[a].dtype)


def field_kernel(s, first, *refs):
    left_ref, out_ref = refs[-2:]
    field = sum(ref[...].astype(F32) for ref in refs[:-2])
    parts = (field.astype(BF),) if first else high_low(field)
    stacked = jnp.concatenate([p.astype(F32) for p in parts], axis=0).astype(BF)
    rows = s.rows
    direct = None
    for k in range(s.kpoints):
        image = lax.dot_general(
            stacked, left_ref[k], (((1,), (1,)), ((), ())), preferred_element_type=F32
        )
        if not first:
            image = image[:rows] + image[rows:]
        own = iota(image.shape, 0) % s.kpoints == k
        direct = jnp.where(own, image, 0.0 if direct is None else direct)
    out_ref[...] = direct


class Sizes:
    pass


VMEM = pl.BlockSpec(memory_space=pltpu.VMEM)
HBM = pl.BlockSpec(memory_space=pltpu.HBM)


def call(body, args, outs, name, specs=None, out_specs=None, scratch=(), limit=24, cost=0):
    return pl.pallas_call(
        body,
        out_shape=[jax.ShapeDtypeStruct(shape, dtype) for shape, dtype in outs],
        in_specs=specs or [VMEM] * len(args),
        out_specs=out_specs or [VMEM] * len(outs),
        scratch_shapes=list(scratch),
        compiler_params=pltpu.CompilerParams(vmem_limit_bytes=limit * 1024 * 1024),
        name=name,
        cost_estimate=pl.CostEstimate(
            flops=cost, bytes_accessed=cost // 256, transcendentals=0
        ),
    )(*args)


def on_device(
    groups, parts,
    energies, current, previous, previous_beta, pair_left, pair_right, screened, momentum_index
):
    s = Sizes()
    s.groups, s.parts, s.chips = groups, parts, parts // CORES
    s.chains, s.kpoints, band_block = current.shape
    s.rows = s.chains * s.kpoints
    s.transfers, width, waves = screened.shape
    bands = pair_left.shape[1]
    nk = momentum_index.shape[0]
    s.entries = float(nk * bands)
    total = groups * s.rows
    state = ((s.rows, bands), F32)
    block = ((s.rows, width), F32)
    pairs = (s.rows * width // CORES // LANES + s.chains) // 2
    packet = ((groups * parts, pairs, 2, LANES), BF)

    def exchange(x, axes):
        return lax.all_to_all(x, axes, 0, 0, tiled=True)

    def across(x, axis, size, distance):
        return lax.ppermute(x, axis, [(i, i ^ distance) for i in range(size)])

    def farthest_first(pieces):
        order = sorted(range(len(pieces)), key=lambda at: -at.bit_count())
        return [pieces[at] for at in order]

    def swap(pieces, axis="kpt"):
        return [pieces[0]] + [
            across(piece, axis, len(pieces), at) for at, piece in enumerate(pieces) if at
        ]

    screened = pltpu.with_memory_space_constraint(screened, pltpu.VMEM)
    inputs = tuple(
        pltpu.with_memory_space_constraint(x, pltpu.HBM)
        for x in (current, previous, energies)
    )
    piece = ((2 * s.rows, 2 * band_block), F32)
    (start,) = call(
        functools.partial(begin_kernel, s),
        inputs,
        [piece],
        "begin",
        specs=[HBM] * len(inputs),
        scratch=[pltpu.VMEM(x.shape, x.dtype) for x in inputs]
        + [pltpu.SemaphoreType.DMA((len(inputs),))],
        cost=COVER,
    )
    (start,) = call(
        functools.partial(stack_kernel, s),
        (start, across(start, "core", CORES, 1)),
        [(((CORES + 1) * s.rows, 2 * band_block), F32)],
        "stack",
    )
    (pick,) = call(
        functools.partial(pick_kernel, s),
        (momentum_index,),
        [((total, s.transfers * 3 * total), BF)],
        "pick",
    )
    start = swap([start] * s.chips, "z")
    sent, vector, earlier, levels, density = call(
        functools.partial(unpack_kernel, s),
        (*start, pair_right, pick),
        [packet, state, state, state, block],
        "unpack",
        cost=COVER,
    )
    scalars = []
    before = work = None
    for step in range(STEPS):
        first, keep = step == 0, step < STEPS - 1
        got = exchange(sent, ("kpt", "z", "core"))
        other = across(got, "core", CORES, 1)
        image = ((s.transfers, total, width), F32)
        (half,) = call(
            functools.partial(half_kernel, s), (got, screened), [image], "half", cost=COVER
        )
        args = (half, got, other) + (() if first else (before,)) + (screened, pick)
        outs = [block] + [((s.rows, width), BF)] * (groups - 1)
        outs += [] if first else [((s.rows, LANES), F32)]
        outs += [image] if keep else []
        results = call(
            functools.partial(screen_kernel, s, first, keep),
            args,
            outs,
            "screen",
            scratch=[pltpu.VMEM((total, width), F32)],
        )
        if not first:
            scalars.append(results[groups])
        if keep:
            before = results[-1]
        (direct,) = call(
            functools.partial(field_kernel, s, first),
            (*farthest_first(swap(results[:groups])), pair_left),
            [state],
            "field",
        )
        (direct,) = call(
            functools.partial(pair_kernel, s),
            (direct, across(direct, "core", CORES, 1)),
            [((s.rows, bands), BF)],
            "pair",
        )
        direct = swap([direct] * s.chips, "z")
        if first:
            sent, work, part = call(
                functools.partial(first_kernel, s),
                (*direct, vector, earlier, levels, previous_beta[None], density, pair_right),
                [packet, state, block],
                "apply",
            )
        elif keep:
            sent, work, vector, *densities = call(
                functools.partial(later_kernel, s),
                (*direct, work, vector, levels, scalars[-1], part, density, pair_right),
                [packet, state, state] + [block, block] * (step < STEPS - 2),
                "apply",
            )
            part, density = densities or (None, None)
        else:
            sent, work, vector = call(
                functools.partial(last_kernel, s),
                (*direct, work, vector, levels, scalars[-1]),
                [((s.rows, LANES), F32), state, state],
                "apply",
            )
    sums = swap([sent] * groups)
    own = (current.shape, F32)
    terms = ((s.chains, STEPS), F32)
    bands_block = ((s.rows, band_block), F32)
    own_work, own_vector, known, prior = call(
        functools.partial(own_kernel, s),
        (work, vector, *scalars),
        [bands_block, bands_block, ((s.rows, LANES), F32), own],
        "own",
        out_specs=[VMEM] * 3 + [HBM],
        scratch=[pltpu.VMEM(*own), pltpu.SemaphoreType.DMA((1,))],
    )
    last, alphas, betas = call(
        functools.partial(end_kernel, s),
        (*sums, own_work, own_vector, known),
        [own, terms, terms],
        "end",
        out_specs=[HBM] * 3,
        scratch=[pltpu.VMEM(*x) for x in (own, terms, terms)]
        + [pltpu.SemaphoreType.DMA((3,))],
    )
    return last, prior, alphas, betas


def solution(mesh):
    groups, parts = mesh.shape["kpt"], mesh.shape["pw"]
    devices = mesh.devices.reshape(groups, parts // CORES, CORES)
    pw = ("z", "core")
    return jax.shard_map(
        functools.partial(on_device, groups, parts),
        mesh=jax.sharding.Mesh(devices, ("kpt", *pw)),
        in_specs=(
            P("kpt", pw),
            P(None, "kpt", pw),
            P(None, "kpt", pw),
            P(),
            P("kpt", None, pw),
            P("kpt", None, pw),
            P("kpt", pw, None),
            P(),
        ),
        out_specs=(P(None, "kpt", pw), P(None, "kpt", pw), P(), P()),
        check_vma=False,
    )
```
